256 devices in a mesh: section: 2 (over core), seq: 16 (over x, y), head: 8 (over z).
Axes of the slice: x: 4, y: 4, z: 8, core: 2. Of those that a mesh axis runs over, the one named last changes fastest.
Arguments:
- x_in: bfloat16 [2, 4096, 8192], P('section', 'seq', 'head'), may hold values from -6 to 6
- b_in: bfloat16 [2, 4096, 2048], P('section', 'seq', 'head'), may hold values from -6 to 6
- c_in: bfloat16 [2, 4096, 2048], P('section', 'seq', 'head'), may hold values from -6 to 6
- z_in: bfloat16 [2, 4096, 8192], P('section', 'seq', 'head'), may hold values from -6 to 6
- dt_raw: float32 [2, 128, 4096], P('section', 'head', 'seq'), may hold values from -5 to 5
- conv_x: float32 [2, 4, 8192], P('section', None, 'head'), may hold values from -3 to 3
- conv_b: float32 [2, 4, 2048], P('section', None, 'head'), may hold values from -3 to 3
- conv_c: float32 [2, 4, 2048], P('section', None, 'head'), may hold values from -3 to 3
- a_rate: float32 [2, 128], P('section', 'head'), may hold values from 0.0001 to 1
- dt_bias: float32 [2, 128], P('section', 'head'), may hold values from -3 to -0.5
- skip_d: float32 [2, 128], P('section', 'head'), may hold values from 0.5 to 2
- norm_gain: float32 [2, 8192], P('section', 'head'), may hold values from 0.25 to 1.75
- out_weight: bfloat16 [2, 8192, 8192], P('section', 'head', 'seq'), may hold values from -0.0625 to 0.0625
Outputs:
- mixed: bfloat16 [2, 4096, 8192], P('section', ('seq', 'head'))
The draws below stay inside these ranges and needn't reach their ends.
All inputs are finite; a program needn't handle non-finite values.
Results may differ from the reference program's by a relative error of at most 0.007.
Values may be sent and summed in bfloat16 or wider, within the bound.
A program may use at most 128 MiB of HBM per device.

```python
import math
import jax
import jax.numpy as jnp
from jax import lax

D = 8192
P_SIZE = 64
N = 256
G = 8
KCONV = 4
HEADS = 128
TOK_DEV = 256
INNER = 8192
TOKENS = 4096
SECTIONS = 2


def draw_a_rate(key, part):
    lowest = math.log(0.0002)
    highest = math.log(1.0)
    exponent = jax.random.uniform(key, (SECTIONS, HEADS), jnp.float32, lowest, highest)
    return jnp.exp(exponent)


def level_of(key, shape, shards, low, top_value):
    level, own = 1.0, jax.random.fold_in(key, 6)
    for position, blocks in shards:
        draws = jnp.exp(jax.random.uniform(jax.random.fold_in(own, position), (blocks,), jnp.float32, low / len(shards), top_value / len(shards)))
        level = level * jnp.repeat(draws, shape[position] // blocks).reshape([-1 if axis == position else 1 for axis in range(len(shape))])
    return level


def gaussian(key, extent, width, bound, pieces=(), kind=jnp.bfloat16):
    gain = level_of(key, extent, pieces, -0.22, 0.18) if pieces else 1.0
    entries = jax.random.normal(key, extent, jnp.float32) * width * gain
    return jnp.minimum(jnp.maximum(entries, -bound), bound).astype(kind)


def setup_inputs(seed: int = 0) -> dict:
    key_of = jax.random.split(jax.random.key(seed), 14)
    return {
        "x_in": gaussian(key_of[0], (SECTIONS, TOKENS, INNER), 1.0, 6.0, ((0, 2), (1, 16), (2, 8))),
        "b_in": gaussian(key_of[1], (SECTIONS, TOKENS, G * N), 1.0, 6.0, ((0, 2), (1, 16), (2, 8))),
        "c_in": gaussian(key_of[2], (SECTIONS, TOKENS, G * N), 1.0, 6.0, ((0, 2), (1, 16), (2, 8))),
        "z_in": gaussian(key_of[3], (SECTIONS, TOKENS, INNER), 1.0, 6.0, ((0, 2), (1, 16), (2, 8))),
        "dt_raw": gaussian(key_of[4], (SECTIONS, HEADS, TOKENS), 1.0, 5.0, ((0, 2), (1, 8), (2, 16)), jnp.float32),
        "conv_x": gaussian(key_of[5], (SECTIONS, KCONV, INNER), KCONV ** -0.5, 3.0, ((0, 2), (2, 8)), jnp.float32),
        "conv_b": gaussian(key_of[6], (SECTIONS, KCONV, G * N), KCONV ** -0.5, 3.0, ((0, 2), (2, 8)), jnp.float32),
        "conv_c": gaussian(key_of[7], (SECTIONS, KCONV, G * N), KCONV ** -0.5, 3.0, ((0, 2), (2, 8)), jnp.float32),
        "a_rate": draw_a_rate(jax.random.fold_in(key_of[13], 71), 0),
        "dt_bias": jnp.clip(-3.0 + 2.5 * jax.random.uniform(key_of[9], (SECTIONS, HEADS), jnp.float32) ** level_of(key_of[9], (SECTIONS, HEADS), ((0, 2), (1, 8)), -0.2, 0.2), -3.0, -0.5),
        "skip_d": jnp.clip(0.5 + 1.5 * jax.random.uniform(key_of[10], (SECTIONS, HEADS), jnp.float32) ** level_of(key_of[10], (SECTIONS, HEADS), ((0, 2), (1, 8)), -0.2, 0.2), 0.5, 2.0),
        "norm_gain": jnp.clip(1.0 + 0.15 * jax.random.normal(key_of[11], (SECTIONS, INNER), jnp.float32), 0.25, 1.75),
        "out_weight": gaussian(key_of[12], (SECTIONS, INNER, D), INNER ** -0.5, 0.0625, ((0, 2), (1, 8), (2, 16))),
    }


epsilon = 1e-05

def conv_silu(signal, kernel):
    kernel_taps = kernel.shape[0]
    length = signal.shape[0]
    padded = jnp.pad(signal, ((kernel_taps - 1, 0), (0, 0)))
    summed = jnp.zeros(signal.shape, jnp.float32)
    for offset in range(kernel_taps):
        summed = summed + kernel[offset] * padded[offset:offset + length].astype(jnp.float32)
    return jax.nn.silu(summed).astype(jnp.bfloat16)

def one_layer(x_in, b_in, c_in, z_in, dt_raw, conv_x, conv_b, conv_c, a_rate, dt_bias, skip_d, norm_gain, out_weight):
    x_conv = conv_silu(x_in, conv_x)
    b_conv = conv_silu(b_in, conv_b)
    c_conv = conv_silu(c_in, conv_c)
    step_size = jax.nn.softplus(dt_raw + dt_bias[:, None])
    step_log = -a_rate[:, None] * step_size
    blocks = TOKENS // TOK_DEV
    per_group = HEADS // G
    x_blocks = x_conv.reshape(blocks, TOK_DEV, G, per_group, P_SIZE)
    b_blocks = b_conv.reshape(blocks, TOK_DEV, G, N)
    c_blocks = c_conv.reshape(blocks, TOK_DEV, G, N)
    z_blocks = z_in.reshape(blocks, TOK_DEV, INNER)
    step_blocks = jnp.transpose(step_size.reshape(G, per_group, blocks, TOK_DEV), (2, 0, 1, 3))
    log_blocks = jnp.transpose(step_log.reshape(G, per_group, blocks, TOK_DEV), (2, 0, 1, 3))
    causal = jnp.arange(TOK_DEV)[:, None] >= jnp.arange(TOK_DEV)[None, :]
    skip_term = skip_d.reshape(G, per_group)

    def block_step(carried, inputs):
        x_block, b_block, c_block, z_block, step_block, log_block = inputs
        log_decay = jnp.cumsum(log_block, axis=2)
        scores = jnp.einsum('tgn,ugn->gtu', c_block.astype(jnp.float32), b_block.astype(jnp.float32))
        spread_log = log_decay[:, :, :, None] - log_decay[:, :, None, :]
        damping = jnp.where(causal, jnp.exp(jnp.minimum(spread_log, 0.0)), 0.0)
        weights = (damping * step_block[:, :, None, :] * scores[:, None]).astype(jnp.bfloat16)
        weights = lax.optimization_barrier(weights).astype(jnp.float32)
        inside = jnp.einsum('gjtu,ugjp->tgjp', weights, x_block.astype(jnp.float32))
        to_end = jnp.exp(log_decay[:, :, -1:] - log_decay) * step_block
        x_weighted = (x_block.astype(jnp.float32) * jnp.transpose(to_end, (2, 0, 1))[..., None]).astype(jnp.bfloat16)
        x_weighted = lax.optimization_barrier(x_weighted).astype(jnp.float32)
        block_sum = jnp.einsum('ugjp,ugn->gjpn', x_weighted, b_block.astype(jnp.float32))
        block_decay = jnp.exp(log_decay[:, :, -1])
        carried_b = lax.optimization_barrier(carried.astype(jnp.bfloat16)).astype(jnp.float32)
        outside = jnp.einsum('tgn,gjpn->tgjp', c_block.astype(jnp.float32), carried_b)
        outside = outside * jnp.transpose(jnp.exp(log_decay), (2, 0, 1))[..., None]
        out_ssm = inside + outside + skip_term[None, :, :, None] * x_block.astype(jnp.float32)
        gated = out_ssm.reshape(TOK_DEV, G, per_group * P_SIZE) * jax.nn.silu(z_block.astype(jnp.float32)).reshape(TOK_DEV, G, per_group * P_SIZE)
        inverse_rms = lax.rsqrt(lax.optimization_barrier(jnp.mean(gated * gated, axis=2, keepdims=True)) + epsilon)
        hidden = ((gated * inverse_rms).reshape(TOK_DEV, INNER) * norm_gain).astype(jnp.bfloat16)
        new_carried = block_decay[:, :, None, None] * carried + block_sum
        return (new_carried, hidden)
    start = jnp.zeros((G, per_group, P_SIZE, N), jnp.float32)
    final_state, hidden = lax.scan(block_step, start, (x_blocks, b_blocks, c_blocks, z_blocks, step_blocks, log_blocks))
    hidden = hidden.reshape(TOKENS, INNER)
    return jnp.dot(hidden, out_weight, preferred_element_type=jnp.float32).astype(jnp.bfloat16)

def reference(x_in, b_in, c_in, z_in, dt_raw, conv_x, conv_b, conv_c, a_rate, dt_bias, skip_d, norm_gain, out_weight):
    layers = []
    for section_index in range(SECTIONS):
        layers.append(one_layer(x_in[section_index], b_in[section_index], c_in[section_index], z_in[section_index], dt_raw[section_index], conv_x[section_index], conv_b[section_index], conv_c[section_index], a_rate[section_index], dt_bias[section_index], skip_d[section_index], norm_gain[section_index], out_weight[section_index]))
    stacked = jnp.stack(layers)
    return jnp.roll(stacked, 1, axis=0)
```

```python
import jax
import jax.numpy as jnp
from jax import lax
from jax.sharding import Mesh
from jax.sharding import PartitionSpec as P
from jax.experimental import pallas as pl
from jax.experimental.pallas import tpu as pltpu

N = 256
SEQ = ("seq_0", "seq_1")
SEQ_HEAD = ("seq_0", "seq_1", "head")


epsilon = 1e-05


def passed_along(block, axis, distance):
    devices = range(lax.axis_size(axis))
    route = [(i - distance, i) for i in devices if i - distance in devices]
    return lax.ppermute(block, axis, route)


def neutral_like(x, identity):
    return jax.tree.map(
        lambda part, zero: jnp.zeros_like(part) + jnp.asarray(zero, part.dtype), x, identity
    )


def entering(x, axes, combine, identity):
    before = start = neutral_like(x, identity)
    so_far = x
    for axis in reversed(axes):
        size, place = (lax.axis_size(axis), lax.axis_index(axis))
        pieces = jax.tree.map(lambda part: lax.all_gather(part, axis), so_far)
        inside, so_far = (start, start)
        for k in range(size):
            passed = k < place
            so_far = combine(so_far, jax.tree.map(lambda part: part[k], pieces))
            inside = jax.tree.map(lambda new, old: jnp.where(passed, new, old), so_far, inside)
        before = combine(inside, before)
    return before


MESH = pl.DeviceIdType.MESH
PIECES = (4, 3, 5, 2, 6, 1, 7, 0)
OFFSETS = (0, 3, 1, 2)


def send(src, dst, send_sem, recv_sem, **to):
    return pltpu.make_async_remote_copy(
        src_ref=src, dst_ref=dst, send_sem=send_sem, recv_sem=recv_sem,
        device_id=to, device_id_type=MESH,
    )


def greet(peers):
    barrier = pltpu.get_barrier_semaphore()
    for peer in peers:
        pl.semaphore_signal(barrier, inc=1, device_id=peer, device_id_type=MESH)
    return lambda: pl.semaphore_wait(barrier, len(peers))


def project_kernel(
    hid, w, out, wg, ag, first_out, first_in, ring_out, ring_in, done,
    w_own, w_send, w_recv, a_send, a_recv, r_send, r_recv, o_send, o_recv,
):
    s, x, y, h = (lax.axis_index(a) for a in ("section", "seq_0", "seq_1", "head"))
    xr, xl = lax.rem(x + 1, 4), lax.rem(x + 3, 4)
    ys = [lax.rem(y + o, 4) for o in OFFSETS]
    up, down = lax.rem(h + 1, 8), lax.rem(h + 7, 8)
    sides = (up, down)
    own = pltpu.make_async_copy(w, wg.at[0], w_own)
    own.start()
    ready = greet(
        [{"seq_1": v} for v in ys[1:]] + [{"seq_0": xr}, {"seq_0": xl}]
        + [{"head": up}, {"head": down}] + [{"section": 1 - s, "seq_1": v} for v in ys]
    )
    for p, k in enumerate(PIECES):
        rows = pl.ds(pl.multiple_of(lax.rem(h + k, 8) * 32, 32), 32)
        ag[p * 128 : p * 128 + 32, :] = hid[rows, :]
    ready()

    def a_direct(p):
        rows = pl.ds(pl.multiple_of(lax.rem(h + PIECES[p], 8) * 32, 32), 32)
        copies = [
            send(hid.at[rows], ag.at[pl.ds(p * 128 + 32, 32)], a_send.at[p, 0], a_recv.at[p, 0], seq_1=ys[2]),
            send(hid.at[rows], ag.at[pl.ds(p * 128 + 64, 32)], a_send.at[p, 1], a_recv.at[p, 1], seq_1=ys[1]),
        ]
        if p == 0:
            copies.append(
                send(hid.at[rows], ag.at[pl.ds(96, 32)], a_send.at[p, 2], a_recv.at[p, 2], seq_1=ys[3])
            )
        return copies

    def a_forward(p):
        return [
            send(ag.at[pl.ds(p * 128 + 32, 16)], ag.at[pl.ds(p * 128 + 96, 16)], a_send.at[p, 2], a_recv.at[p, 2], seq_1=ys[2]),
            send(ag.at[pl.ds(p * 128 + 80, 16)], ag.at[pl.ds(p * 128 + 112, 16)], a_send.at[p, 3], a_recv.at[p, 3], seq_1=ys[1]),
        ]

    started = []

    def start(copies):
        for c in copies:
            c.start()
        started.extend(copies)
        return copies

    direct = {p: a_direct(p) for p in range(8)}
    passed = {p: a_forward(p) for p in range(1, 8)}
    start(direct[0])
    w_direct = start([
        send(w, wg.at[1], w_send.at[0], w_recv.at[0], seq_0=xr),
        send(w, wg.at[2], w_send.at[1], w_recv.at[1], seq_0=xl),
    ])
    start(direct[1])
    start(direct[2])
    own.wait()

    def forward(p):
        direct[p][0].wait_recv()
        passed_now = passed[p]
        start(passed_now[:1])
        direct[p][1].wait_recv()
        start(passed_now[1:])

    def arrived(p):
        for c in passed[p]:
            c.wait_recv()

    def ring(stage, j, side):
        src, dst = (first_out, first_in) if stage == 0 else (ring_out, ring_in)
        at = (side, j) if stage == 0 else (side, stage - 1, j)
        axis = {"head": sides[side]}
        return send(src.at[at], dst.at[at], r_send.at[side, stage, j], r_recv.at[side, stage, j], **axis)

    for c in direct[0]:
        c.wait_recv()

    def first(j, _):
        part = jnp.dot(ag[0:128, :], wg[j], preferred_element_type=jnp.float32)
        first_out[0, j] = part[:, :256].astype(jnp.bfloat16)
        first_out[1, j] = part[:, 256:].astype(jnp.bfloat16)
        ring(0, j, 0).start()
        ring(0, j, 1).start()
        return 0

    first(0, 0)
    for c in w_direct:
        c.wait_recv()
    w_passed = start([
        send(wg.at[1, pl.ds(0, 512)], wg.at[3, pl.ds(0, 512)], w_send.at[2], w_recv.at[2], seq_0=xr),
        send(wg.at[2, pl.ds(512, 512)], wg.at[3, pl.ds(512, 512)], w_send.at[3], w_recv.at[3], seq_0=xl),
    ])
    lax.fori_loop(1, 3, first, 0)
    for c in w_passed:
        c.wait_recv()
    first(3, 0)
    forward(1)
    forward(2)

    for stage in (1, 2, 3):
        p = 2 * stage - 1
        start(direct[p + 2])
        if stage < 3:
            start(direct[p + 3])
        arrived(p)
        arrived(p + 1)

        def middle(j, _):
            part = jnp.dot(ag[p * 128 : p * 128 + 256, :], wg[j], preferred_element_type=jnp.float32)
            for side in (0, 1):
                mine = part[side * 128 : side * 128 + 128]
                ring(stage - 1, j, side).wait_recv()
                if stage == 1:
                    got = first_in[side, j].astype(jnp.float32)
                    if side == 0:
                        ring_out[side, 0, j, :, :256] = (mine[:, :256] + got).astype(jnp.bfloat16)
                        ring_out[side, 0, j, :, 256:] = mine[:, 256:].astype(jnp.bfloat16)
                    else:
                        ring_out[side, 0, j, :, :256] = mine[:, :256].astype(jnp.bfloat16)
                        ring_out[side, 0, j, :, 256:] = (mine[:, 256:] + got).astype(jnp.bfloat16)
                else:
                    got = ring_in[side, stage - 2, j].astype(jnp.float32)
                    ring_out[side, stage - 1, j] = (mine + got).astype(jnp.bfloat16)
            ring(stage, j, 0).start()
            ring(stage, j, 1).start()
            return 0

        lax.fori_loop(0, 4, middle, 0)
        forward(p + 2)
        if stage < 3:
            forward(p + 3)

    arrived(7)
    results = []
    for j in range(4):
        part = jnp.dot(ag[896:1024, :], wg[j], preferred_element_type=jnp.float32)
        for side in (0, 1):
            ring(3, j, side).wait_recv()
        total = part + ring_in[0, 2, j].astype(jnp.float32) + ring_in[1, 2, j].astype(jnp.float32)
        done[j] = total.astype(jnp.bfloat16)
        column = (lax.rem(x + OFFSETS[j], 4) * 4 + y) * 512
        cols = pl.ds(pl.multiple_of(column, 512), 512)
        for r in range(4):
            results.append(
                send(done.at[j, pl.ds(r * 32, 32)], out.at[:, cols], o_send.at[r, j], o_recv.at[r, j], section=1 - s, seq_1=ys[r])
            )
        for c in results[-4:]:
            c.start()

    for c in started:
        c.wait_send()
    for stage in range(4):

        def drain(j, _):
            ring(stage, j, 0).wait_send()
            ring(stage, j, 1).wait_send()
            return 0

        lax.fori_loop(0, 4, drain, 0)
    for c in results:
        c.wait_send()
        c.wait_recv()


def project(hidden, weight):
    dma = pltpu.SemaphoreType.DMA
    vmem = lambda *shape: pltpu.VMEM(shape, jnp.bfloat16)
    return pl.pallas_call(
        project_kernel,
        out_shape=jax.ShapeDtypeStruct((32, 8192), jnp.bfloat16),
        in_specs=[pl.BlockSpec(memory_space=pltpu.VMEM), pl.BlockSpec(memory_space=pl.ANY)],
        out_specs=pl.BlockSpec(memory_space=pl.ANY),
        scratch_shapes=[
            vmem(4, 1024, 512), vmem(1024, 1024),
            vmem(2, 4, 128, 256), vmem(2, 4, 128, 256),
            vmem(2, 3, 4, 128, 512), vmem(2, 3, 4, 128, 512), vmem(4, 128, 512),
            dma, dma((4,)), dma((4,)), dma((8, 4)), dma((8, 4)),
            dma((2, 4, 4)), dma((2, 4, 4)), dma((4, 4)), dma((4, 4)),
        ],
        compiler_params=pltpu.CompilerParams(
            collective_id=0, has_side_effects=True, vmem_limit_bytes=48 * 2**20
        ),
    )(hidden, weight)


def conv_silu(padded, kernel, length):
    kernel_taps = kernel.shape[0]
    summed = jnp.zeros((length, padded.shape[1]), jnp.float32)
    for offset in range(kernel_taps):
        summed = summed + kernel[offset] * padded[offset : offset + length].astype(jnp.float32)
    return jax.nn.silu(summed).astype(jnp.bfloat16)


def carry_combine(earlier, latter):
    return (earlier[0] * latter[0], latter[0][:, :, None, None] * earlier[1] + latter[1])


def per_device(
    x_in,
    b_in,
    c_in,
    z_in,
    dt_raw,
    conv_x,
    conv_b,
    conv_c,
    a_rate,
    dt_bias,
    skip_d,
    norm_gain,
    out_weight,
):
    x_local = x_in[0]
    b_local = b_in[0]
    c_local = c_in[0]
    length = x_local.shape[0]
    kernel_taps = conv_x.shape[1]
    x_cols = x_local.shape[1]
    b_cols = b_local.shape[1]
    edge_rows = jnp.concatenate(
        [
            x_local[length - kernel_taps + 1 :],
            b_local[length - kernel_taps + 1 :],
            c_local[length - kernel_taps + 1 :],
        ],
        axis=1,
    )
    before = passed_along(edge_rows, SEQ, 1)
    x_conv = conv_silu(jnp.concatenate([before[:, :x_cols], x_local], axis=0), conv_x[0], length)
    b_conv = conv_silu(
        jnp.concatenate([before[:, x_cols : x_cols + b_cols], b_local], axis=0), conv_b[0], length
    )
    c_conv = conv_silu(
        jnp.concatenate([before[:, x_cols + b_cols :], c_local], axis=0), conv_c[0], length
    )
    head_count = dt_raw.shape[1]
    group_count = b_cols // N
    per_group = head_count // group_count
    head_dim = x_cols // head_count
    step_size = jax.nn.softplus(dt_raw[0] + dt_bias[0][:, None])
    log_decay = jnp.cumsum(-a_rate[0][:, None] * step_size, axis=1)
    x_groups = x_conv.reshape(length, group_count, per_group, head_dim)
    b_groups = b_conv.reshape(length, group_count, N)
    c_groups = c_conv.reshape(length, group_count, N)
    log_groups = log_decay.reshape(group_count, per_group, length)
    step_groups = step_size.reshape(group_count, per_group, length)
    scores = jnp.einsum("tgn,ugn->gtu", c_groups, b_groups, preferred_element_type=jnp.float32)
    causal = jnp.arange(length)[:, None] >= jnp.arange(length)[None, :]
    spread_log = log_groups[:, :, :, None] - log_groups[:, :, None, :]
    damping = jnp.where(causal, jnp.exp(jnp.minimum(spread_log, 0.0)), 0.0)
    weights = (damping * step_groups[:, :, None, :] * scores[:, None]).astype(jnp.bfloat16)
    inside = jnp.einsum("gjtu,ugjp->tgjp", weights, x_groups, preferred_element_type=jnp.float32)
    to_end = jnp.exp(log_groups[:, :, -1:] - log_groups) * step_groups
    x_weighted = (
        x_groups.astype(jnp.float32) * jnp.transpose(to_end, (2, 0, 1))[..., None]
    ).astype(jnp.bfloat16)
    block_sum = jnp.einsum(
        "ugjp,ugn->gjpn", x_weighted, b_groups, preferred_element_type=jnp.float32
    )
    block_decay = jnp.exp(log_groups[:, :, -1])
    identity = (jnp.ones_like(block_decay), jnp.zeros_like(block_sum))
    carried_decay, carried = entering((block_decay, block_sum), SEQ, carry_combine, identity)
    carried_b = carried.astype(jnp.bfloat16)
    outside = jnp.einsum("tgn,gjpn->tgjp", c_groups, carried_b, preferred_element_type=jnp.float32)
    outside = outside * jnp.transpose(jnp.exp(log_groups), (2, 0, 1))[..., None]
    skip_term = skip_d[0].reshape(group_count, per_group)
    out_ssm = inside + outside + skip_term[None, :, :, None] * x_groups.astype(jnp.float32)
    gate_act = jax.nn.silu(z_in[0].astype(jnp.float32)).reshape(
        length, group_count, per_group * head_dim
    )
    gated = out_ssm.reshape(length, group_count, per_group * head_dim) * gate_act
    inverse_rms = lax.rsqrt(jnp.mean(gated * gated, axis=2, keepdims=True) + epsilon)
    hidden = ((gated * inverse_rms).reshape(length, x_cols) * norm_gain[0]).astype(jnp.bfloat16)
    local_weight = out_weight[0]
    passed = project(hidden, local_weight)
    return passed[None]


def solution(mesh):
    finer = Mesh(
        mesh.devices.reshape(mesh.shape["section"], 4, 4, mesh.shape["head"]),
        ("section", "seq_0", "seq_1", "head"),
    )
    return jax.shard_map(
        per_device,
        mesh=finer,
        in_specs=(
            P("section", SEQ, "head"),
            P("section", SEQ, "head"),
            P("section", SEQ, "head"),
            P("section", SEQ, "head"),
            P("section", "head", SEQ),
            P("section", None, "head"),
            P("section", None, "head"),
            P("section", None, "head"),
            P("section", "head"),
            P("section", "head"),
            P("section", "head"),
            P("section", "head"),
            P("section", "head", SEQ),
        ),
        out_specs=P("section", SEQ_HEAD, None),
        check_vma=False,
    )
```

```python
import jax
import jax.numpy as jnp
from jax import lax
from jax.experimental import pallas as pl
from jax.experimental.pallas import tpu as pltpu
from jax.sharding import Mesh
from jax.sharding import PartitionSpec as P

SEQ = ("seq_0", "seq_1")
SEQ_HEAD = ("seq_0", "seq_1", "head")
MESH = pl.DeviceIdType.MESH
PIECES = (4, 3, 5, 2, 6, 1, 7, 0)
OFFSETS = (0, 3, 1, 2)
PEERS = tuple((dx, dy) for dx in (2, 1, 3, 0) for dy in (2, 1, 3, 0) if dx or dy)
W_CUTS = (0, 256, 512, 1024)
F32 = jnp.float32
BF16 = jnp.bfloat16

epsilon = 1e-05


def send(src, dst, send_sem, recv_sem, **to):
    return pltpu.make_async_remote_copy(
        src_ref=src, dst_ref=dst, send_sem=send_sem, recv_sem=recv_sem,
        device_id=to, device_id_type=MESH,
    )


def exact_dot(a, b):
    return jnp.dot(a, b, precision=lax.Precision.HIGHEST, preferred_element_type=F32)


def conv_blocks(padded, kernel, out, blocks):
    def columns(i, _):
        cols = pl.ds(pl.multiple_of(i * 256, 256), 256)
        for block in blocks:
            summed = jnp.zeros((64, 256), F32)
            for k in range(4):
                summed = summed + kernel[k : k + 1, cols] * padded[block * 64 + 5 + k : block * 64 + 69 + k, cols]
            out[block * 64 : block * 64 + 64, cols] = (summed * jax.nn.sigmoid(summed)).astype(BF16)
        return 0

    lax.fori_loop(0, out.shape[1] // 256, columns, 0)


def mixer_kernel(
    x_in, b_in, c_in, z_in, dt, conv_x, conv_b, conv_c, rate, bias, skip, gain, w, out,
    halo_x, halo_b, halo_c, pad_x, pad_b, pad_c, xc, bc, cc, xw,
    step, logd, decay_own, decay, state, state_in, state_out, carried, scores, inside, grow, to_end,
    wg, ag, ring_out, ring_in, done,
    h_send, h_recv, d_send, d_recv, s_send, s_recv, t_send, t_recv,
    w_own, w_send, w_recv, wf_send, wf_recv, a_send, a_recv, r_send, r_recv, o_send, o_recv,
):
    s, x, y, h = (lax.axis_index(a) for a in ("section", "seq_0", "seq_1", "head"))
    q = x * 4 + y
    xr, xl = lax.rem(x + 1, 4), lax.rem(x + 3, 4)
    ys = [lax.rem(y + o, 4) for o in OFFSETS]
    sides = (lax.rem(h + 1, 8), lax.rem(h + 7, 8))
    peers = [(lax.rem(x + dx, 4), lax.rem(y + dy, 4)) for dx, dy in PEERS]

    barrier = pltpu.get_barrier_semaphore()
    greeted = (
        [{"seq_0": u, "seq_1": v} for u, v in peers]
        + [{"head": v} for v in sides]
        + [{"section": 1 - s, "seq_1": v} for v in ys]
    )
    for peer in greeted:
        pl.semaphore_signal(barrier, inc=1, device_id=peer, device_id_type=MESH)

    own_w = pltpu.make_async_copy(w, wg.at[0], w_own)
    own_w.start()

    started = []

    def start(copies):
        for c in copies:
            c.start()
        started.extend(copies)
        return copies

    row16 = lax.broadcasted_iota(jnp.int32, (16, 16), 0)
    col16 = lax.broadcasted_iota(jnp.int32, (16, 16), 1)

    def column(row):
        return jnp.sum(jnp.where(row16 == col16, jnp.broadcast_to(row, (16, 16)), 0.0), axis=1, keepdims=True)

    raw = dt[...] + column(bias[...])
    step_size = jnp.maximum(raw, 0.0) + jnp.log1p(jnp.exp(-jnp.abs(raw)))
    log_decay = -column(rate[...]) * step_size
    lane = lax.broadcasted_iota(jnp.int32, (16, 256), 1)
    for shift in (1, 2, 4, 8, 16, 32, 64, 128):
        log_decay = log_decay + jnp.where(lane >= shift, pltpu.roll(log_decay, shift, 1), 0.0)
    step[...] = step_size
    logd[...] = log_decay
    spread = jnp.where(
        lax.shift_right_logical(lax.broadcasted_iota(jnp.int32, (16, 1024), 1), 6)
        == lax.broadcasted_iota(jnp.int32, (16, 1024), 0), 1.0, 0.0,
    ).astype(F32)
    log_cols = log_decay.T
    end_cols = (jnp.exp(log_decay[:, 255:256] - log_decay) * step_size).T
    last = exact_dot(jnp.exp(log_cols[248:256, :]), spread)[7:8, :]
    for r in range(8):
        decay_own[r : r + 1, :] = last[:, r * 128 : r * 128 + 128]
    decay[q] = decay_own[...]

    pl.semaphore_wait(barrier, len(greeted))

    to_next = {"seq_0": lax.rem(x + lax.div(y + 1, 4), 4), "seq_1": lax.rem(y + 1, 4)}
    halo = start([
        send(src.at[pl.ds(240, 16)], dst, h_send.at[i], h_recv.at[i], **to_next)
        for i, (src, dst) in enumerate(((b_in, halo_b), (x_in, halo_x), (c_in, halo_c)))
    ])
    decays = start([
        send(decay_own, decay.at[q], d_send.at[i], d_recv.at[i], seq_0=u, seq_1=v)
        for i, (u, v) in enumerate(peers)
    ])

    def w_part(i):
        n = W_CUTS[i + 1] - W_CUTS[i]
        plus, minus = pl.ds(W_CUTS[i], n), pl.ds(1024 - W_CUTS[i + 1], n)
        return [
            send(w.at[plus], wg.at[1, plus], w_send.at[0, i], w_recv.at[0, i], seq_0=xr),
            send(w.at[minus], wg.at[2, minus], w_send.at[1, i], w_recv.at[1, i], seq_0=xl),
        ]

    w_direct = [start(w_part(0))]

    pad_x[8:264, :] = x_in[...].astype(F32)
    pad_b[8:264, :] = b_in[...].astype(F32)
    pad_c[8:264, :] = c_in[...].astype(F32)
    to_end[...] = exact_dot(end_cols, spread)
    conv_blocks(pad_b, conv_b, bc, (1, 2, 3))
    conv_blocks(pad_x, conv_x, xc, (1, 2, 3))

    def finish(i, halo_ref, padded, kernel, conv_out):
        halo[i].wait_recv()
        padded[0:8, :] = jnp.where(q > 0, halo_ref[...].astype(F32)[8:16], 0.0)
        conv_blocks(padded, kernel, conv_out, (0,))

    finish(0, halo_b, pad_b, conv_b, bc)
    finish(1, halo_x, pad_x, conv_x, xc)

    b_cols = bc[...].astype(F32).T.astype(BF16)
    for i in range(4):
        cols = slice(i * 256, i * 256 + 256)
        xw[:, cols] = (xc[:, cols].astype(F32) * to_end[:, cols]).astype(BF16)
        state[:, cols] = jnp.dot(b_cols, xw[:, cols], preferred_element_type=F32).astype(BF16)
    state_in[q] = state[pl.ds(pl.multiple_of(q * 16, 16), 16), :]
    sums = start([
        send(
            state.at[pl.ds(pl.multiple_of((u * 4 + v) * 16, 16), 16)], state_in.at[q],
            s_send.at[i], s_recv.at[i], seq_0=u, seq_1=v,
        )
        for i, (u, v) in enumerate(peers)
    ])
    w_direct.append(start(w_part(1)))

    conv_blocks(pad_c, conv_c, cc, (1, 2, 3))
    finish(2, halo_c, pad_c, conv_c, cc)
    scores[...] = lax.dot_general(cc[...], bc[...], (((1,), (1,)), ((), ())), preferred_element_type=F32)
    skip_row = exact_dot(jnp.broadcast_to(skip[...], (8, 16)), spread)[0:1, :]
    causal = lax.broadcasted_iota(jnp.int32, (128, 128), 0) >= lax.broadcasted_iota(jnp.int32, (128, 128), 1)
    first_half = lax.broadcasted_iota(jnp.int32, (256, 128), 1) < 64
    grow_cols = jnp.exp(log_cols)

    def damped(log_col, head, rows, cols, masked):
        value = jnp.exp(jnp.minimum(log_col[rows] - logd[head : head + 1, cols], 0.0))
        if masked:
            value = jnp.where(causal, value, 0.0)
        return (value * step[head : head + 1, cols] * scores[rows, cols]).astype(BF16)

    top, bottom = slice(0, 128), slice(128, 256)

    def pair(g):
        lanes = slice(g * 128, g * 128 + 128)
        parts = []
        for head in (2 * g, 2 * g + 1):
            log_col = log_cols[:, head : head + 1]
            upper = jnp.dot(damped(log_col, head, top, top, True), xc[top, lanes], preferred_element_type=F32)
            lower = jnp.dot(damped(log_col, head, bottom, top, False), xc[top, lanes], preferred_element_type=F32)
            lower = lower + jnp.dot(damped(log_col, head, bottom, bottom, True), xc[bottom, lanes], preferred_element_type=F32)
            parts.append(jnp.concatenate([upper, lower], axis=0))
        both = jnp.where(first_half, parts[0], parts[1])
        zf = z_in[:, lanes].astype(F32)
        gate = zf * jax.nn.sigmoid(zf)
        inside[:, lanes] = (both + skip_row[:, lanes] * xc[:, lanes].astype(F32)) * gate
        grow[:, lanes] = exact_dot(grow_cols, spread[:, lanes]) * gate

    for g in range(4):
        pair(g)

    for c in decays + sums:
        c.wait_recv()
    for r in range(8):
        lanes = slice(r * 128, r * 128 + 128)
        acc = jnp.zeros((16, 128), F32)
        for k in range(16):
            state_out[k, :, lanes] = acc.astype(BF16)
            if k < 15:
                acc = decay[k, r : r + 1, :] * acc + state_in[k, :, lanes].astype(F32)
    my_rows = pl.ds(pl.multiple_of(q * 16, 16), 16)
    entering = start([
        send(state_out.at[u * 4 + v], carried.at[my_rows], t_send.at[i], t_recv.at[i], seq_0=u, seq_1=v)
        for i, (u, v) in enumerate(peers)
    ])
    carried[my_rows, :] = state_out[q]
    w_direct.append(start(w_part(2)))

    for g in range(4, 8):
        pair(g)
    for side in (0, 1):
        for j in range(4):
            ring_in[side, 0, j, :, 256 - 256 * side : 512 - 256 * side] = jnp.zeros((128, 256), BF16)

    def w_forward(i):
        n = W_CUTS[i + 1] - W_CUTS[i]
        plus, minus = pl.ds(W_CUTS[i], n), pl.ds(1024 - W_CUTS[i + 1], n)
        return [
            send(wg.at[1, plus], wg.at[3, plus], wf_send.at[0, i], wf_recv.at[0, i], seq_0=xr),
            send(wg.at[2, minus], wg.at[3, minus], wf_send.at[1, i], wf_recv.at[1, i], seq_0=xl),
        ]

    w_passed = []

    def forward_w(i):
        for c in w_direct[i]:
            c.wait_recv()
        w_passed.extend(start(w_forward(i)))

    def a_direct(p):
        mine = ag.at[pl.ds(p * 128, 32)]
        copies = [
            send(mine, ag.at[pl.ds(p * 128 + 32, 32)], a_send.at[p, 0], a_recv.at[p, 0], seq_1=ys[2]),
            send(mine, ag.at[pl.ds(p * 128 + 64, 32)], a_send.at[p, 1], a_recv.at[p, 1], seq_1=ys[1]),
        ]
        if p == 0:
            copies.append(send(mine, ag.at[pl.ds(96, 32)], a_send.at[p, 2], a_recv.at[p, 2], seq_1=ys[3]))
        return copies

    def a_forward(p):
        return [
            send(ag.at[pl.ds(p * 128 + 32, 16)], ag.at[pl.ds(p * 128 + 96, 16)], a_send.at[p, 2], a_recv.at[p, 2], seq_1=ys[2]),
            send(ag.at[pl.ds(p * 128 + 80, 16)], ag.at[pl.ds(p * 128 + 112, 16)], a_send.at[p, 3], a_recv.at[p, 3], seq_1=ys[1]),
        ]

    direct = {p: a_direct(p) for p in range(8)}
    passed = {p: a_forward(p) for p in range(1, 8)}

    for c in entering:
        c.wait_recv()

    def hidden(p):
        rows = pl.ds(pl.multiple_of(lax.rem(h + PIECES[p], 8) * 32, 32), 32)
        outside = jnp.dot(cc[rows, :], carried[...], preferred_element_type=F32)
        gated = inside[rows, :] + outside * grow[rows, :]
        inverse_rms = lax.rsqrt(jnp.mean(gated * gated, axis=1, keepdims=True) + epsilon)
        ag[p * 128 : p * 128 + 32, :] = (gated * inverse_rms * gain[...]).astype(BF16)

    hidden(0)
    hidden(1)
    start(direct[0])
    hidden(2)
    start(direct[1])
    hidden(3)
    start(direct[2])
    for p in range(4, 8):
        hidden(p)
    own_w.wait()
    forward_w(0)

    def forward(p):
        direct[p][0].wait_recv()
        start(passed[p][:1])
        direct[p][1].wait_recv()
        start(passed[p][1:])

    def arrived(p):
        for c in passed[p]:
            c.wait_recv()

    def ring(stage, j, side):
        axis = {"head": sides[side]}
        src, dst = ring_out.at[side, stage, j], ring_in.at[side, stage, j]
        if stage == 0:
            half = pl.ds(side * 256, 256)
            src, dst = src.at[:, half], dst.at[:, half]
        return send(src, dst, r_send.at[side, stage, j], r_recv.at[side, stage, j], **axis)

    rings = {(stage, j): [ring(stage, j, side) for side in (0, 1)] for stage in range(4) for j in range(4)}

    def first(j):
        part = jnp.dot(ag[0:128, :], wg[j], preferred_element_type=F32)
        ring_out[0, 0, j, :, :256] = part[:, :256].astype(BF16)
        ring_out[1, 0, j, :, 256:] = part[:, 256:].astype(BF16)
        start(rings[0, j])

    def middle(stage, j):
        p = 2 * stage - 1
        part = jnp.dot(ag[p * 128 : p * 128 + 256, :], wg[j], preferred_element_type=F32)
        for side in (0, 1):
            rings[stage - 1, j][side].wait_recv()
            got = ring_in[side, stage - 1, j].astype(F32)
            ring_out[side, stage, j] = (part[side * 128 : side * 128 + 128] + got).astype(BF16)
        start(rings[stage, j])

    results = []

    def final(j):
        part = jnp.dot(ag[896:1024, :], wg[j], preferred_element_type=F32)
        for side in (0, 1):
            rings[3, j][side].wait_recv()
        total = part + ring_in[0, 3, j].astype(F32) + ring_in[1, 3, j].astype(F32)
        done[j] = total.astype(BF16)
        cols = pl.ds(pl.multiple_of((lax.rem(x + OFFSETS[j], 4) * 4 + y) * 512, 512), 512)
        copies = [
            send(done.at[j, pl.ds(r * 32, 32)], out.at[:, cols], o_send.at[r, j], o_recv.at[r, j], section=1 - s, seq_1=ys[r])
            for r in range(4)
        ]
        results.extend(start(copies))

    for c in direct[0]:
        c.wait_recv()
    first(0)
    forward_w(1)
    for c in w_direct[2]:
        c.wait_recv()
    first(1)
    first(2)
    forward(1)
    forward(2)
    start(direct[3])
    start(direct[4])
    arrived(1)
    arrived(2)
    for j in range(3):
        middle(1, j)
    forward(3)
    forward(4)
    start(direct[5])
    start(direct[6])
    for c in w_passed:
        c.wait_recv()
    first(3)
    arrived(3)
    arrived(4)
    for j in range(3):
        middle(2, j)
    forward(5)
    forward(6)
    start(direct[7])
    middle(1, 3)
    arrived(5)
    arrived(6)
    for j in range(3):
        middle(3, j)
    forward(7)
    middle(2, 3)
    middle(3, 3)
    arrived(7)
    for j in range(4):
        final(j)

    for c in started:
        c.wait_send()
    for c in results:
        c.wait_recv()


def per_device(
    x_in, b_in, c_in, z_in, dt_raw, conv_x, conv_b, conv_c, a_rate, dt_bias, skip_d, norm_gain, out_weight
):
    dma = pltpu.SemaphoreType.DMA
    half = lambda *shape: pltpu.VMEM(shape, BF16)
    full = lambda *shape: pltpu.VMEM(shape, F32)
    in_vmem = pl.BlockSpec(memory_space=pltpu.VMEM)
    anywhere = pl.BlockSpec(memory_space=pl.ANY)
    mixed = pl.pallas_call(
        mixer_kernel,
        out_shape=jax.ShapeDtypeStruct((32, 8192), BF16),
        in_specs=[in_vmem] * 12 + [anywhere],
        out_specs=anywhere,
        scratch_shapes=[
            half(16, 1024), half(16, 256), half(16, 256), full(264, 1024), full(264, 256), full(264, 256),
            half(256, 1024), half(256, 256), half(256, 256), half(256, 1024),
            full(16, 256), full(16, 256), full(8, 128), full(16, 8, 128),
            half(256, 1024), half(16, 16, 1024), half(16, 16, 1024), half(256, 1024),
            full(256, 256), full(256, 1024), full(256, 1024), full(256, 1024),
            half(4, 1024, 512), half(1024, 1024), half(2, 4, 4, 128, 512), half(2, 4, 4, 128, 512), half(4, 128, 512),
            dma((3,)), dma((3,)), dma((15,)), dma((15,)), dma((15,)), dma((15,)), dma((15,)), dma((15,)),
            dma, dma((2, 3)), dma((2, 3)), dma((2, 2)), dma((2, 2)), dma((8, 4)), dma((8, 4)),
            dma((2, 4, 4)), dma((2, 4, 4)), dma((4, 4)), dma((4, 4)),
        ],
        compiler_params=pltpu.CompilerParams(
            collective_id=0, has_side_effects=True, vmem_limit_bytes=56 * 2**20
        ),
    )(
        x_in[0], b_in[0], c_in[0], z_in[0], dt_raw[0], conv_x[0], conv_b[0], conv_c[0],
        a_rate, dt_bias, skip_d, norm_gain, out_weight[0],
    )
    return mixed[None]


def solution(mesh):
    finer = Mesh(
        mesh.devices.reshape(mesh.shape["section"], 4, 4, mesh.shape["head"]),
        ("section", "seq_0", "seq_1", "head"),
    )
    return jax.shard_map(
        per_device,
        mesh=finer,
        in_specs=(
            P("section", SEQ, "head"),
            P("section", SEQ, "head"),
            P("section", SEQ, "head"),
            P("section", SEQ, "head"),
            P("section", "head", SEQ),
            P("section", None, "head"),
            P("section", None, "head"),
            P("section", None, "head"),
            P("section", "head"),
            P("section", "head"),
            P("section", "head"),
            P("section", "head"),
            P("section", "head", SEQ),
        ),
        out_specs=P("section", SEQ_HEAD, None),
        check_vma=False,
    )
```

```python
import jax
import jax.numpy as jnp
from jax import lax
from jax.experimental import pallas as pl
from jax.experimental.pallas import tpu as pltpu
from jax.sharding import Mesh
from jax.sharding import PartitionSpec as P

SEQ = ("seq_0", "seq_1")
SEQ_HEAD = ("seq_0", "seq_1", "head")
MESH = pl.DeviceIdType.MESH
PIECES = (4, 3, 5, 2, 6, 1, 7, 0)
OFFSETS = (0, 3, 1, 2)
PEERS = tuple((dx, dy) for dx in (2, 1, 3, 0) for dy in (2, 1, 3, 0) if dx or dy)
W_CUTS = (0, 336, 672, 1024)
ROWS = ((0, 32), (32, 64), (96, 32), (0, 128))
F32 = jnp.float32
BF16 = jnp.bfloat16

epsilon = 1e-05


def send(src, dst, send_sem, recv_sem, **to):
    return pltpu.make_async_remote_copy(
        src_ref=src, dst_ref=dst, send_sem=send_sem, recv_sem=recv_sem,
        device_id=to, device_id_type=MESH,
    )


def exact_dot(a, b):
    return jnp.dot(a, b, precision=lax.Precision.HIGHEST, preferred_element_type=F32)


def conv_blocks(padded, kernel, out, blocks):
    def columns(i, _):
        cols = pl.ds(pl.multiple_of(i * 256, 256), 256)
        for block in blocks:
            summed = jnp.zeros((64, 256), F32)
            for k in range(4):
                summed = summed + kernel[k : k + 1, cols] * padded[block * 64 + 5 + k : block * 64 + 69 + k, cols]
            out[block * 64 : block * 64 + 64, cols] = (summed * jax.nn.sigmoid(summed)).astype(BF16)
        return 0

    lax.fori_loop(0, out.shape[1] // 256, columns, 0)


def mixer_kernel(
    x_hbm, b_hbm, c_hbm, z_hbm, dt_hbm, conv_x_hbm, conv_b_hbm, conv_c_hbm, rate_hbm, bias_hbm, skip_hbm, gain_hbm, w, out,
    x_in, b_in, c_in, z_in, dt, conv_x, conv_b, conv_c, rate, bias, skip, gain,
    halo_x, halo_b, halo_c, pad_x, pad_b, pad_c, xc, bc, cc, xw,
    step, logd, decay_own, decay, state, state_in, state_out, carried, scores, inside, grow, to_end,
    wg, ag, ring_out, ring_in, done,
    l_sem, h_send, h_recv, d_sem, s_sem, t_sem,
    w_own, w_send, w_recv, wf_send, wf_recv, f_send, f_recv, a_send, a_recv, r_send, r_recv, o_sem,
):
    s, x, y, h = (lax.axis_index(a) for a in ("section", "seq_0", "seq_1", "head"))
    q = x * 4 + y
    ring_at = [[lax.rem(v + o, 4) for o in OFFSETS] for v in (x, y)]
    sides = (lax.rem(h + 1, 8), lax.rem(h + 7, 8))
    peers = [(lax.rem(x + dx, 4), lax.rem(y + dy, 4)) for dx, dy in PEERS]

    barrier = pltpu.get_barrier_semaphore()
    greeted = (
        [{"seq_0": u, "seq_1": v} for u, v in peers]
        + [{"head": v} for v in sides]
        + [{"section": 1 - s, "seq_1": v} for v in ring_at[1]]
        + [{"section": 1 - s, "seq_0": v} for v in ring_at[0][1:]]
    )
    for peer in greeted:
        pl.semaphore_signal(barrier, inc=1, device_id=peer, device_id_type=MESH)

    loads = {}
    for i, (name, src, dst) in enumerate((
        ("dt", dt_hbm, dt), ("bias", bias_hbm, bias), ("rate", rate_hbm, rate),
        ("b", b_hbm, b_in), ("x", x_hbm, x_in), ("c", c_hbm, c_in),
        ("kb", conv_b_hbm, conv_b), ("kx", conv_x_hbm, conv_x), ("kc", conv_c_hbm, conv_c),
        ("skip", skip_hbm, skip), ("z", z_hbm, z_in), ("gain", gain_hbm, gain),
    )):
        loads[name] = pltpu.make_async_copy(src, dst, l_sem.at[i])
        loads[name].start()
    own_w = [pltpu.make_async_copy(w.at[:, pl.ds(a * 256, 256)], wg.at[a, 0], w_own.at[a]) for a in (0, 1)]
    for c in own_w:
        c.start()

    def loaded(*names):
        for n in names:
            loads[n].wait()

    def all_of(ref, sem):
        pltpu.make_async_copy(ref, ref, sem).wait()

    def start(copies):
        for c in copies:
            c.start()

    loaded("dt", "bias", "rate")
    row16 = lax.broadcasted_iota(jnp.int32, (16, 16), 0)
    col16 = lax.broadcasted_iota(jnp.int32, (16, 16), 1)

    def column(row):
        return jnp.sum(jnp.where(row16 == col16, jnp.broadcast_to(row, (16, 16)), 0.0), axis=1, keepdims=True)

    raw = dt[...] + column(bias[...])
    step_size = jnp.maximum(raw, 0.0) + jnp.log1p(jnp.exp(-jnp.abs(raw)))
    log_decay = -column(rate[...]) * step_size
    lane = lax.broadcasted_iota(jnp.int32, (16, 256), 1)
    for shift in (1, 2, 4, 8, 16, 32, 64, 128):
        log_decay = log_decay + jnp.where(lane >= shift, pltpu.roll(log_decay, shift, 1), 0.0)
    step[...] = step_size
    logd[...] = log_decay
    spread = jnp.where(
        lax.shift_right_logical(lax.broadcasted_iota(jnp.int32, (16, 1024), 1), 6)
        == lax.broadcasted_iota(jnp.int32, (16, 1024), 0), 1.0, 0.0,
    ).astype(F32)
    log_cols = log_decay.T
    end_cols = (jnp.exp(log_decay[:, 255:256] - log_decay) * step_size).T
    last = exact_dot(jnp.exp(log_cols[248:256, :]), spread)[7:8, :]
    for r in range(8):
        decay_own[r : r + 1, :] = last[:, r * 128 : r * 128 + 128]
    decay[q] = decay_own[...]

    loaded("b", "x", "c")
    pl.semaphore_wait(barrier, len(greeted))

    to_next = {"seq_0": lax.rem(x + lax.div(y + 1, 4), 4), "seq_1": lax.rem(y + 1, 4)}
    halo = [
        send(src.at[pl.ds(240, 16)], dst, h_send.at[i], h_recv.at[i], **to_next)
        for i, (src, dst) in enumerate(((b_in, halo_b), (x_in, halo_x), (c_in, halo_c)))
    ]

    @pl.when(q < 15)
    def _():
        for c in halo:
            c.start()

    start([
        send(decay_own, decay.at[q], d_sem.at[0], d_sem.at[1], seq_0=u, seq_1=v)
        for i, (u, v) in enumerate(peers)
    ])

    def w_part(i):
        n = W_CUTS[i + 1] - W_CUTS[i]
        plus, minus = pl.ds(W_CUTS[i], n), pl.ds(1024 - W_CUTS[i + 1], n)
        copies = []
        for a in (0, 1):
            cols = pl.ds(a * 256, 256)
            copies += [
                send(w.at[plus, cols], wg.at[a, 1, plus], w_send, w_recv.at[a, 0], **{SEQ[a]: ring_at[a][2]}),
                send(w.at[minus, cols], wg.at[a, 2, minus], w_send, w_recv.at[a, 1], **{SEQ[a]: ring_at[a][1]}),
            ]
        return copies

    start(w_part(0))

    loaded("kb", "kx", "kc", "skip", "z", "gain")
    pad_x[8:264, :] = x_in[...].astype(F32)
    pad_b[8:264, :] = b_in[...].astype(F32)
    pad_c[8:264, :] = c_in[...].astype(F32)
    to_end[...] = exact_dot(end_cols, spread)
    conv_blocks(pad_b, conv_b, bc, (1, 2, 3))
    conv_blocks(pad_x, conv_x, xc, (1, 2, 3))

    def finish(i, halo_ref, padded, kernel, conv_out):
        @pl.when(q > 0)
        def _():
            halo[i].wait_recv()
            padded[0:8, :] = halo_ref[...].astype(F32)[8:16]

        @pl.when(q == 0)
        def _():
            padded[0:8, :] = jnp.zeros((8, padded.shape[1]), F32)

        conv_blocks(padded, kernel, conv_out, (0,))

    finish(0, halo_b, pad_b, conv_b, bc)
    finish(1, halo_x, pad_x, conv_x, xc)

    b_cols = bc[...].astype(F32).T.astype(BF16)
    for i in range(4):
        cols = slice(i * 256, i * 256 + 256)
        xw[:, cols] = (xc[:, cols].astype(F32) * to_end[:, cols]).astype(BF16)
        state[:, cols] = jnp.dot(b_cols, xw[:, cols], preferred_element_type=F32).astype(BF16)
    state_in[q] = state[pl.ds(pl.multiple_of(q * 16, 16), 16), :]
    start([
        send(
            state.at[pl.ds(pl.multiple_of((u * 4 + v) * 16, 16), 16)], state_in.at[q],
            s_sem.at[0], s_sem.at[1], seq_0=u, seq_1=v,
        )
        for i, (u, v) in enumerate(peers)
    ])
    start(w_part(1))

    conv_blocks(pad_c, conv_c, cc, (1, 2, 3))
    finish(2, halo_c, pad_c, conv_c, cc)
    scores[...] = lax.dot_general(cc[...], bc[...], (((1,), (1,)), ((), ())), preferred_element_type=F32)
    skip_row = exact_dot(jnp.broadcast_to(skip[...], (8, 16)), spread)[0:1, :]
    causal = lax.broadcasted_iota(jnp.int32, (128, 128), 0) >= lax.broadcasted_iota(jnp.int32, (128, 128), 1)
    first_half = lax.broadcasted_iota(jnp.int32, (256, 128), 1) < 64
    grow_cols = jnp.exp(log_cols)

    def damped(log_col, head, rows, cols, masked):
        value = jnp.exp(jnp.minimum(log_col[rows] - logd[head : head + 1, cols], 0.0))
        if masked:
            value = jnp.where(causal, value, 0.0)
        return (value * step[head : head + 1, cols] * scores[rows, cols]).astype(BF16)

    top, bottom = slice(0, 128), slice(128, 256)

    def pair(g):
        lanes = slice(g * 128, g * 128 + 128)
        parts = []
        for head in (2 * g, 2 * g + 1):
            log_col = log_cols[:, head : head + 1]
            upper = jnp.dot(damped(log_col, head, top, top, True), xc[top, lanes], preferred_element_type=F32)
            lower = jnp.dot(damped(log_col, head, bottom, top, False), xc[top, lanes], preferred_element_type=F32)
            lower = lower + jnp.dot(damped(log_col, head, bottom, bottom, True), xc[bottom, lanes], preferred_element_type=F32)
            parts.append(jnp.concatenate([upper, lower], axis=0))
        both = jnp.where(first_half, parts[0], parts[1])
        zf = z_in[:, lanes].astype(F32)
        gate = zf * jax.nn.sigmoid(zf)
        inside[:, lanes] = (both + skip_row[:, lanes] * xc[:, lanes].astype(F32)) * gate
        grow[:, lanes] = exact_dot(grow_cols, spread[:, lanes]) * gate

    for g in range(4):
        pair(g)

    all_of(decay.at[pl.ds(0, 15)], d_sem.at[1])
    all_of(state.at[pl.ds(0, 240)], s_sem.at[1])
    for r in range(8):
        lanes = slice(r * 128, r * 128 + 128)
        acc = jnp.zeros((16, 128), F32)
        for k in range(16):
            state_out[k, :, lanes] = acc.astype(BF16)
            if k < 15:
                acc = decay[k, r : r + 1, :] * acc + state_in[k, :, lanes].astype(F32)
    my_rows = pl.ds(pl.multiple_of(q * 16, 16), 16)
    start([
        send(state_out.at[u * 4 + v], carried.at[my_rows], t_sem.at[0], t_sem.at[1], seq_0=u, seq_1=v)
        for i, (u, v) in enumerate(peers)
    ])
    carried[my_rows, :] = state_out[q]

    start(w_part(2))

    def w_forward():
        plus, minus = pl.ds(0, 512), pl.ds(512, 512)
        copies = []
        for a in (0, 1):
            copies += [
                send(wg.at[a, 1, plus], wg.at[a, 3, plus], wf_send, wf_recv.at[a], **{SEQ[a]: ring_at[a][2]}),
                send(wg.at[a, 2, minus], wg.at[a, 3, minus], wf_send, wf_recv.at[a], **{SEQ[a]: ring_at[a][1]}),
            ]
        return copies

    for g in range(4, 8):
        pair(g)
    for side in (0, 1):
        for j in range(4):
            ring_in[side, 0, j, :, 256 - 256 * side : 512 - 256 * side] = jnp.zeros((128, 256), BF16)

    def a_direct(p):
        copies = []
        for a in (0, 1):
            mine, all_rows = ag.at[a, pl.ds(p * 128, 32)], ag.at[a]
            axis, to = SEQ[1 - a], ring_at[1 - a]
            copies += [
                send(mine, all_rows.at[pl.ds(p * 128 + 32, 32)], a_send.at[0], a_recv.at[0, p], **{axis: to[2]}),
                send(mine, all_rows.at[pl.ds(p * 128 + 64, 32)], a_send.at[0], a_recv.at[0, p], **{axis: to[1]}),
            ]
        return copies

    def a_forward(p):
        copies = []
        for a in (0, 1):
            rows = ag.at[a]
            axis, to = SEQ[1 - a], ring_at[1 - a]
            copies += [
                send(rows.at[pl.ds(p * 128 + 32, 16)], rows.at[pl.ds(p * 128 + 96, 16)], a_send.at[1], a_recv.at[1, p], **{axis: to[2]}),
                send(rows.at[pl.ds(p * 128 + 80, 16)], rows.at[pl.ds(p * 128 + 112, 16)], a_send.at[1], a_recv.at[1, p], **{axis: to[1]}),
            ]
        return copies

    direct = {p: a_direct(p) for p in range(8)}
    passed = {p: a_forward(p) for p in range(8)}

    all_of(state.at[pl.ds(0, 240)], t_sem.at[1])

    def hidden(p):
        rows = pl.ds(pl.multiple_of(lax.rem(h + PIECES[p], 8) * 32, 32), 32)
        outside = jnp.dot(cc[rows, :], carried[...], preferred_element_type=F32)
        gated = inside[rows, :] + outside * grow[rows, :]
        inverse_rms = lax.rsqrt(jnp.mean(gated * gated, axis=1, keepdims=True) + epsilon)
        value = (gated * inverse_rms * gain[...]).astype(BF16)
        ag[0, p * 128 : p * 128 + 32, :] = value
        ag[1, p * 128 : p * 128 + 32, :] = value

    hidden(0)
    start(direct[0])
    hidden(1)
    start(direct[1])
    hidden(2)
    start(direct[2])
    for p in range(3, 8):
        hidden(p)
    for c in own_w:
        c.wait()

    def forward(p):
        all_of(ag.at[0, pl.ds(0, 128)], a_recv.at[0, p])
        start(passed[p])

    def arrived(p):
        all_of(ag.at[0, pl.ds(0, 64)], a_recv.at[1, p])

    def ring(stage, j, side):
        src, dst = ring_out.at[side, stage, j], ring_in.at[side, stage, j]
        return send(src, dst, r_send, r_recv.at[stage - 1, j], **{"head": sides[side]})

    def ring_first(j, side, group):
        low, size = ROWS[group]
        rows, half = pl.ds(low, size), pl.ds(side * 256, 256)
        return send(
            ring_out.at[side, 0, j, rows, half], ring_in.at[side, 0, j, rows, half],
            f_send, f_recv.at[j], **{"head": sides[side]},
        )

    rings = {(stage, j): [[ring(stage, j, side)] for side in (0, 1)] for stage in (1, 2, 3) for j in range(4)}
    for j in range(4):
        groups = (3,) if j == 3 else (0, 1, 2)
        rings[0, j] = [[ring_first(j, side, g) for g in groups] for side in (0, 1)]

    def first(j, group):
        low, size = ROWS[group]
        for a in (0, 1):
            part = jnp.dot(ag[a, low : low + size, :], wg[a, j], preferred_element_type=F32)
            ring_out[a, 0, j, low : low + size, a * 256 : a * 256 + 256] = part.astype(BF16)
        for side in (0, 1):
            start([rings[0, j][side][group % 3]])

    def middle(stage, j):
        p = 2 * stage - 1
        parts = [jnp.dot(ag[a, p * 128 : p * 128 + 256, :], wg[a, j], preferred_element_type=F32) for a in (0, 1)]
        if stage == 1:
            all_of(ring_in.at[0, 0, j], f_recv.at[j])
        else:
            all_of(ring_in.at[0, 0, pl.ds(0, 2)], r_recv.at[stage - 2, j])
        for side in (0, 1):
            for a in (0, 1):
                cols = slice(a * 256, a * 256 + 256)
                got = ring_in[side, stage - 1, j, :, cols].astype(F32)
                ring_out[side, stage, j, :, cols] = (parts[a][side * 128 : side * 128 + 128] + got).astype(BF16)
        start(rings[stage, j][0] + rings[stage, j][1])

    def final(j):
        parts = [jnp.dot(ag[a, 896:1024, :], wg[a, j], preferred_element_type=F32) for a in (0, 1)]
        all_of(ring_in.at[0, 0, pl.ds(0, 2)], r_recv.at[2, j])
        for a in (0, 1):
            half = slice(a * 256, a * 256 + 256)
            total = parts[a] + ring_in[0, 3, j, :, half].astype(F32) + ring_in[1, 3, j, :, half].astype(F32)
            done[a, j] = total.astype(BF16)
        copies = []
        for a in (0, 1):
            shard = ring_at[0][j] * 4 + y if a == 0 else x * 4 + ring_at[1][j]
            cols = pl.ds(pl.multiple_of(shard * 512 + a * 256, 256), 256)
            for r in (3, 1, 2, 0):
                axis = {SEQ[1 - a]: ring_at[1 - a][r]}
                copies.append(
                    send(done.at[a, j, pl.ds(r * 32, 32)], out.at[:, cols], o_sem.at[0], o_sem.at[1], section=1 - s, **axis)
                )
        start(copies)

    first(0, 0)
    for a in (0, 1):
        for side in (0, 1):
            all_of(wg.at[a, 1 + side], w_recv.at[a, side])
    first(1, 0)
    first(2, 0)
    forward(0)
    for j in range(3):
        first(j, 1)
    forward(1)
    forward(2)
    start(w_forward())
    arrived(0)
    for j in range(3):
        first(j, 2)
    start(direct[3])
    start(direct[4])
    arrived(1)
    arrived(2)
    for j in range(3):
        middle(1, j)
        if j > 0:
            forward(2 + j)
            start(direct[4 + j])
    for a in (0, 1):
        all_of(wg.at[a, 3], wf_recv.at[a])
    first(3, 3)
    arrived(3)
    arrived(4)
    for stage, j in ((2, 0), (2, 1), (1, 3), (2, 2)):
        middle(stage, j)
        if stage == 2 and j > 0:
            forward(4 + j)
    start(direct[7])
    arrived(5)
    arrived(6)
    for stage, j in ((3, 0), (2, 3), (3, 1), (3, 2), (3, 3)):
        middle(stage, j)
        if stage == 3 and j == 1:
            forward(7)
    arrived(7)
    for j in range(4):
        final(j)

    all_of(decay.at[pl.ds(0, 15)], d_sem.at[0])
    all_of(state.at[pl.ds(0, 240)], s_sem.at[0])
    all_of(state.at[pl.ds(0, 240)], t_sem.at[0])
    all_of(ag.at[0], w_send)
    all_of(ag.at[0, pl.ds(0, 512)], wf_send)
    all_of(ag.at[0, pl.ds(0, 256)], f_send)
    all_of(ag.at[0], a_send.at[0])
    all_of(ag.at[0, pl.ds(0, 512)], a_send.at[1])
    all_of(ring_out.at[:, pl.ds(1, 3)], r_send)
    all_of(done, o_sem.at[0])

    @pl.when(q < 15)
    def _():
        for c in halo:
            c.wait_send()

    all_of(out, o_sem.at[1])


def per_device(
    x_in, b_in, c_in, z_in, dt_raw, conv_x, conv_b, conv_c, a_rate, dt_bias, skip_d, norm_gain, out_weight
):
    dma = pltpu.SemaphoreType.DMA
    half = lambda *shape: pltpu.VMEM(shape, BF16)
    full = lambda *shape: pltpu.VMEM(shape, F32)
    anywhere = pl.BlockSpec(memory_space=pl.ANY)
    mixed = pl.pallas_call(
        mixer_kernel,
        out_shape=jax.ShapeDtypeStruct((32, 8192), BF16),
        in_specs=[anywhere] * 13,
        out_specs=anywhere,
        scratch_shapes=[
            half(256, 1024), half(256, 256), half(256, 256), half(256, 1024), full(16, 256),
            full(4, 1024), full(4, 256), full(4, 256), full(1, 16), full(1, 16), full(1, 16), full(1, 1024),
            half(16, 1024), half(16, 256), half(16, 256), full(264, 1024), full(264, 256), full(264, 256),
            half(256, 1024), half(256, 256), half(256, 256), half(256, 1024),
            full(16, 256), full(16, 256), full(8, 128), full(16, 8, 128),
            half(256, 1024), half(16, 16, 1024), half(16, 16, 1024), half(256, 1024),
            full(256, 256), full(256, 1024), full(256, 1024), full(256, 1024),
            half(2, 4, 1024, 256), half(2, 1024, 1024), half(2, 4, 4, 128, 512), half(2, 4, 4, 128, 512), half(2, 4, 128, 256),
            dma((12,)), dma((3,)), dma((3,)), dma((2,)), dma((2,)), dma((2,)),
            dma((2,)), dma, dma((2, 2)), dma, dma((2,)), dma, dma((4,)), dma((2,)), dma((2, 8)), dma, dma((3, 4)), dma((2,)),
        ],
        compiler_params=pltpu.CompilerParams(
            collective_id=0, has_side_effects=True, vmem_limit_bytes=56 * 2**20
        ),
    )(
        x_in[0], b_in[0], c_in[0], z_in[0], dt_raw[0], conv_x[0], conv_b[0], conv_c[0],
        a_rate, dt_bias, skip_d, norm_gain, out_weight[0],
    )
    return mixed[None]


def solution(mesh):
    finer = Mesh(
        mesh.devices.reshape(mesh.shape["section"], 4, 4, mesh.shape["head"]),
        ("section", "seq_0", "seq_1", "head"),
    )
    return jax.shard_map(
        per_device,
        mesh=finer,
        in_specs=(
            P("section", SEQ, "head"),
            P("section", SEQ, "head"),
            P("section", SEQ, "head"),
            P("section", SEQ, "head"),
            P("section", "head", SEQ),
            P("section", None, "head"),
            P("section", None, "head"),
            P("section", None, "head"),
            P("section", "head"),
            P("section", "head"),
            P("section", "head"),
            P("section", "head"),
            P("section", "head", SEQ),
        ),
        out_specs=P("section", SEQ_HEAD, None),
        check_vma=False,
    )
```

```python
import jax
import jax.numpy as jnp
from jax import lax
from jax.experimental import pallas as pl
from jax.experimental.pallas import tpu as pltpu
from jax.sharding import Mesh
from jax.sharding import PartitionSpec as P

SEQ = ("seq_0", "seq_1")
SEQ_HEAD = ("seq_0", "seq_1", "head")
MESH = pl.DeviceIdType.MESH
PIECES = (4, 3, 5, 2, 6, 1, 7, 0)
OFFSETS = (0, 3, 1, 2)
PEERS = tuple((dx, dy) for dx in (2, 1, 3, 0) for dy in (2, 1, 3, 0) if dx or dy)
W_CUT = 672
UNITS = ((0, None), (1, 0), (2, 0), (1, 1), (2, 1), (3, 0), (3, 1))
ALL, NEAR, FAR, OWN, SIDE = (0, 128), (0, 96), (96, 32), (0, 32), (32, 64)
F32 = jnp.float32
ORDER = (
    ("hd", 0), ("hd", 2), ("first", 0, OWN), ("first", 2, OWN), ("hd", 1), ("first", 1, OWN),
    ("hd", 3), ("hd", 4), ("first", 2, SIDE), ("fw", 0), ("wb",), ("first", 0, SIDE),
    ("first", 1, SIDE), ("fw", 1), ("fw", 2), ("wf", 0), ("mid", 1, 2, NEAR), ("mid", 1, 0, NEAR),
    ("first", 0, FAR), ("first", 1, FAR), ("mid", 1, 1, NEAR), ("mid", 2, 2, NEAR), ("first", 2, FAR), ("fw", 3),
    ("mid", 2, 0, NEAR), ("first", 4, ALL), ("mid", 2, 1, NEAR), ("fw", 4), ("first", 3, ALL), ("wf", 1),
    ("mid", 1, 2, FAR), ("mid", 1, 0, FAR), ("hd", 6), ("mid", 1, 1, FAR), ("mid", 1, 4, ALL), ("first", 5, ALL),
    ("mid", 1, 3, ALL), ("mid", 2, 2, FAR), ("mid", 2, 0, FAR), ("mid", 2, 1, FAR), ("hd", 5), ("first", 6, ALL),
    ("mid", 1, 5, ALL), ("mid", 2, 3, ALL), ("fw", 5), ("mid", 2, 4, ALL), ("fw", 6), ("mid", 1, 6, ALL),
    ("mid", 2, 5, ALL), ("mid", 3, 0, ALL), ("hd", 7), ("mid", 3, 1, ALL), ("mid", 2, 6, ALL), ("fw", 7),
    ("mid", 3, 5, ALL), ("mid", 3, 2, ALL), ("mid", 3, 4, ALL), ("mid", 3, 3, ALL), ("mid", 3, 6, ALL), ("fin", 0),
    ("fin", 4), ("fin", 2), ("fin", 1), ("fin", 5), ("fin", 3), ("fin", 6),
)
BF16 = jnp.bfloat16

SPLIT = 2
SPLIT_UNITS = 3
epsilon = 1e-05


def send(src, dst, send_sem, recv_sem, **to):
    return pltpu.make_async_remote_copy(
        src_ref=src, dst_ref=dst, send_sem=send_sem, recv_sem=recv_sem,
        device_id=to, device_id_type=MESH,
    )


def exact_dot(a, b):
    return jnp.dot(a, b, precision=lax.Precision.HIGHEST, preferred_element_type=F32)


def conv_blocks(padded, kernel, out, blocks):
    def columns(i, _):
        cols = pl.ds(pl.multiple_of(i * 256, 256), 256)
        for block in blocks:
            summed = jnp.zeros((64, 256), F32)
            for k in range(4):
                summed = summed + kernel[k : k + 1, cols] * padded[block * 64 + 5 + k : block * 64 + 69 + k, cols]
            out[block * 64 : block * 64 + 64, cols] = (summed * jax.nn.sigmoid(summed)).astype(BF16)
        return 0

    lax.fori_loop(0, out.shape[1] // 256, columns, 0)


def mixer_kernel(
    x_hbm, b_hbm, c_hbm, z_hbm, dt_hbm, conv_x_hbm, conv_b_hbm, conv_c_hbm, rate_hbm, bias_hbm, skip_hbm, gain_hbm, w, out,
    x_in, b_in, c_in, z_in, dt, conv_x, conv_b, conv_c, rate, bias, skip, gain,
    halo_x, halo_b, halo_c, pad_x, pad_b, pad_c, xc, bc, cc, xw,
    step, logd, decay_own, decay, state, state_in, state_out, carried, scores, inside, grow, to_end,
    wg, ag, ring_out, ring_in, done,
    l_sem, h_send, h_recv, d_sem, s_sem, t_sem,
    w_own, w_send, w_recv, wf_send, wf_recv, f_send, f_recv, a_send, a_recv, r_send, r_recv, o_sem,
):
    s, x, y, h = (lax.axis_index(a) for a in ("section", "seq_0", "seq_1", "head"))
    q = x * 4 + y
    ring_at = [[lax.rem(v + o, 4) for o in OFFSETS] for v in (x, y)]
    sides = (lax.rem(h + 1, 8), lax.rem(h + 7, 8))
    peers = [(lax.rem(x + dx, 4), lax.rem(y + dy, 4)) for dx, dy in PEERS]

    barrier = pltpu.get_barrier_semaphore()
    greeted = (
        [{"seq_0": u, "seq_1": v} for u, v in peers]
        + [{"head": v} for v in sides]
        + [{"section": 1 - s, "seq_1": v} for v in ring_at[1]]
        + [{"section": 1 - s, "seq_0": v} for v in ring_at[0][1:]]
    )
    for peer in greeted:
        pl.semaphore_signal(barrier, inc=1, device_id=peer, device_id_type=MESH)

    loads = {}
    for i, (name, src, dst) in enumerate((
        ("dt", dt_hbm, dt), ("bias", bias_hbm, bias), ("rate", rate_hbm, rate),
        ("b", b_hbm, b_in), ("x", x_hbm, x_in), ("c", c_hbm, c_in),
        ("kb", conv_b_hbm, conv_b), ("kx", conv_x_hbm, conv_x), ("kc", conv_c_hbm, conv_c),
        ("skip", skip_hbm, skip), ("z", z_hbm, z_in), ("gain", gain_hbm, gain),
    )):
        loads[name] = pltpu.make_async_copy(src, dst, l_sem.at[i])
        loads[name].start()
    own_w = [pltpu.make_async_copy(w.at[:, pl.ds(a * 256, 256)], wg.at[a, 0], w_own.at[a]) for a in (0, 1)]
    for c in own_w:
        c.start()

    def loaded(*names):
        for n in names:
            loads[n].wait()

    def all_of(ref, sem):
        pltpu.make_async_copy(ref, ref, sem).wait()

    def start(copies):
        for c in copies:
            c.start()

    loaded("dt", "bias", "rate")
    row16 = lax.broadcasted_iota(jnp.int32, (16, 16), 0)
    col16 = lax.broadcasted_iota(jnp.int32, (16, 16), 1)

    def column(row):
        return jnp.sum(jnp.where(row16 == col16, jnp.broadcast_to(row, (16, 16)), 0.0), axis=1, keepdims=True)

    raw = dt[...] + column(bias[...])
    step_size = jnp.maximum(raw, 0.0) + jnp.log1p(jnp.exp(-jnp.abs(raw)))
    log_decay = -column(rate[...]) * step_size
    lane = lax.broadcasted_iota(jnp.int32, (16, 256), 1)
    for shift in (1, 2, 4, 8, 16, 32, 64, 128):
        log_decay = log_decay + jnp.where(lane >= shift, pltpu.roll(log_decay, shift, 1), 0.0)
    step[...] = step_size
    logd[...] = log_decay
    spread = jnp.where(
        lax.shift_right_logical(lax.broadcasted_iota(jnp.int32, (16, 1024), 1), 6)
        == lax.broadcasted_iota(jnp.int32, (16, 1024), 0), 1.0, 0.0,
    ).astype(F32)
    log_cols = log_decay.T
    end_cols = (jnp.exp(log_decay[:, 255:256] - log_decay) * step_size).T
    last = exact_dot(jnp.exp(log_cols[248:256, :]), spread)[7:8, :]
    for r in range(8):
        decay_own[r : r + 1, :] = last[:, r * 128 : r * 128 + 128]
    decay[q] = decay_own[...]

    loaded("b", "x", "c")
    pl.semaphore_wait(barrier, len(greeted))

    to_next = {"seq_0": lax.rem(x + lax.div(y + 1, 4), 4), "seq_1": lax.rem(y + 1, 4)}
    halo = [
        send(src.at[pl.ds(240, 16)], dst, h_send.at[i], h_recv.at[i], **to_next)
        for i, (src, dst) in enumerate(((b_in, halo_b), (x_in, halo_x), (c_in, halo_c)))
    ]

    @pl.when(q < 15)
    def _():
        for c in halo:
            c.start()

    start([
        send(decay_own, decay.at[q], d_sem.at[0], d_sem.at[1], seq_0=u, seq_1=v)
        for i, (u, v) in enumerate(peers)
    ])

    def w_direct(b, low, size, sems):
        rows = pl.ds(low, size)
        copies = []
        for a in (0, 1):
            for slot, to in ((1, 2), (2, 1)):
                copies.append(send(
                    w.at[rows, pl.ds(a * 256 + b * 128, 128)], wg.at[a, slot, rows, pl.ds(b * 128, 128)],
                    sems[0], sems[1], **{SEQ[a]: ring_at[a][to]},
                ))
        return copies

    start(w_direct(0, 0, W_CUT, (w_send, w_recv.at[0])))

    loaded("kb", "kx", "kc", "skip", "z", "gain")
    pad_x[8:264, :] = x_in[...].astype(F32)
    pad_b[8:264, :] = b_in[...].astype(F32)
    pad_c[8:264, :] = c_in[...].astype(F32)
    to_end[...] = exact_dot(end_cols, spread)
    conv_blocks(pad_b, conv_b, bc, (1, 2, 3))
    conv_blocks(pad_x, conv_x, xc, (1, 2, 3))

    def finish(i, halo_ref, padded, kernel, conv_out):
        @pl.when(q > 0)
        def _():
            halo[i].wait_recv()
            padded[0:8, :] = halo_ref[...].astype(F32)[8:16]

        @pl.when(q == 0)
        def _():
            padded[0:8, :] = jnp.zeros((8, padded.shape[1]), F32)

        conv_blocks(padded, kernel, conv_out, (0,))

    finish(0, halo_b, pad_b, conv_b, bc)
    finish(1, halo_x, pad_x, conv_x, xc)

    b_cols = bc[...].astype(F32).T.astype(BF16)
    for i in range(4):
        cols = slice(i * 256, i * 256 + 256)
        xw[:, cols] = (xc[:, cols].astype(F32) * to_end[:, cols]).astype(BF16)
        state[:, cols] = jnp.dot(b_cols, xw[:, cols], preferred_element_type=F32).astype(BF16)
    state_in[q] = state[pl.ds(pl.multiple_of(q * 16, 16), 16), :]
    start([
        send(
            state.at[pl.ds(pl.multiple_of((u * 4 + v) * 16, 16), 16)], state_in.at[q],
            s_sem.at[0], s_sem.at[1], seq_0=u, seq_1=v,
        )
        for i, (u, v) in enumerate(peers)
    ])
    start(w_direct(0, W_CUT, 1024 - W_CUT, (w_send, w_recv.at[0])))

    conv_blocks(pad_c, conv_c, cc, (1, 2, 3))
    finish(2, halo_c, pad_c, conv_c, cc)
    scores[...] = lax.dot_general(cc[...], bc[...], (((1,), (1,)), ((), ())), preferred_element_type=F32)
    skip_row = exact_dot(jnp.broadcast_to(skip[...], (8, 16)), spread)[0:1, :]
    causal = lax.broadcasted_iota(jnp.int32, (128, 128), 0) >= lax.broadcasted_iota(jnp.int32, (128, 128), 1)
    first_half = lax.broadcasted_iota(jnp.int32, (256, 128), 1) < 64
    grow_cols = jnp.exp(log_cols)

    def damped(log_col, head, rows, cols, masked):
        value = jnp.exp(jnp.minimum(log_col[rows] - logd[head : head + 1, cols], 0.0))
        if masked:
            value = jnp.where(causal, value, 0.0)
        return (value * step[head : head + 1, cols] * scores[rows, cols]).astype(BF16)

    top, bottom = slice(0, 128), slice(128, 256)

    def pair(g):
        lanes = slice(g * 128, g * 128 + 128)
        parts = []
        for head in (2 * g, 2 * g + 1):
            log_col = log_cols[:, head : head + 1]
            upper = jnp.dot(damped(log_col, head, top, top, True), xc[top, lanes], preferred_element_type=F32)
            lower = jnp.dot(damped(log_col, head, bottom, top, False), xc[top, lanes], preferred_element_type=F32)
            lower = lower + jnp.dot(damped(log_col, head, bottom, bottom, True), xc[bottom, lanes], preferred_element_type=F32)
            parts.append(jnp.concatenate([upper, lower], axis=0))
        both = jnp.where(first_half, parts[0], parts[1])
        zf = z_in[:, lanes].astype(F32)
        gate = zf * jax.nn.sigmoid(zf)
        inside[:, lanes] = (both + skip_row[:, lanes] * xc[:, lanes].astype(F32)) * gate
        grow[:, lanes] = exact_dot(grow_cols, spread[:, lanes]) * gate

    for g in range(4):
        pair(g)

    all_of(decay.at[pl.ds(0, 15)], d_sem.at[1])
    all_of(state.at[pl.ds(0, 240)], s_sem.at[1])
    for r in range(8):
        lanes = slice(r * 128, r * 128 + 128)
        acc = jnp.zeros((16, 128), F32)
        for k in range(16):
            state_out[k, :, lanes] = acc.astype(BF16)
            if k < 15:
                acc = decay[k, r : r + 1, :] * acc + state_in[k, :, lanes].astype(F32)
    my_rows = pl.ds(pl.multiple_of(q * 16, 16), 16)
    start([
        send(state_out.at[u * 4 + v], carried.at[my_rows], t_sem.at[0], t_sem.at[1], seq_0=u, seq_1=v)
        for i, (u, v) in enumerate(peers)
    ])
    carried[my_rows, :] = state_out[q]

    def w_forward(b):
        cols = pl.ds(b * 128, 128)
        copies = []
        for a in (0, 1):
            for slot, to, low in ((1, 2, 0), (2, 1, 512)):
                at = (pl.ds(low, 512), cols)
                copies.append(send(
                    wg.at[(a, slot, *at)], wg.at[(a, 3, *at)], wf_send, wf_recv.at[b], **{SEQ[a]: ring_at[a][to]},
                ))
        return copies

    for g in range(4, 8):
        pair(g)
    for side in (0, 1):
        for j in range(4):
            for b in (0, 1):
                at = b * 256 + (1 - side) * 128
                ring_in[side, 0, j, :, at : at + 128] = jnp.zeros((128, 128), BF16)
    def a_direct(p):
        copies = []
        for a in (0, 1):
            mine, all_rows = ag.at[a, pl.ds(p * 128, 32)], ag.at[a]
            axis, to = SEQ[1 - a], ring_at[1 - a]
            copies += [
                send(mine, all_rows.at[pl.ds(p * 128 + 32, 32)], a_send.at[0], a_recv.at[0, p], **{axis: to[2]}),
                send(mine, all_rows.at[pl.ds(p * 128 + 64, 32)], a_send.at[0], a_recv.at[0, p], **{axis: to[1]}),
            ]
        return copies

    def a_forward(p):
        copies = []
        for a in (0, 1):
            rows = ag.at[a]
            axis, to = SEQ[1 - a], ring_at[1 - a]
            copies += [
                send(rows.at[pl.ds(p * 128 + 32, 16)], rows.at[pl.ds(p * 128 + 96, 16)], a_send.at[1], a_recv.at[1, p], **{axis: to[2]}),
                send(rows.at[pl.ds(p * 128 + 80, 16)], rows.at[pl.ds(p * 128 + 112, 16)], a_send.at[1], a_recv.at[1, p], **{axis: to[1]}),
            ]
        return copies

    direct = {p: a_direct(p) for p in range(8)}
    passed = {p: a_forward(p) for p in range(8)}

    all_of(state.at[pl.ds(0, 240)], t_sem.at[1])

    def hidden(p):
        rows = pl.ds(pl.multiple_of(lax.rem(h + PIECES[p], 8) * 32, 32), 32)
        outside = jnp.dot(cc[rows, :], carried[...], preferred_element_type=F32)
        gated = inside[rows, :] + outside * grow[rows, :]
        inverse_rms = lax.rsqrt(jnp.mean(gated * gated, axis=1, keepdims=True) + epsilon)
        value = (gated * inverse_rms * gain[...]).astype(BF16)
        ag[0, p * 128 : p * 128 + 32, :] = value
        ag[1, p * 128 : p * 128 + 32, :] = value

    seen = set()

    def need(key):
        if key in seen:
            return
        seen.add(key)
        kind, index = key
        if kind == "own":
            for c in own_w:
                c.wait()
        if kind == "direct":
            all_of(ag.at[0, pl.ds(0, 128)], a_recv.at[0, index])
        if kind == "passed":
            all_of(ag.at[0, pl.ds(0, 64)], a_recv.at[1, index])
        if kind == "w":
            all_of(ag.at[0, pl.ds(0, 512)], w_recv.at[index])
        if kind == "wf":
            all_of(ag.at[0, pl.ds(0, 256)], wf_recv.at[index])

    def need_rows(p, group):
        need(("direct", p))
        if group in (ALL, FAR):
            need(("passed", p))

    def need_w(u):
        j, b = UNITS[u]
        need(("own", 0))
        if j in (1, 2):
            need(("w", b))
        if j == 3:
            need(("wf", b))

    def unit_cols(u):
        b = UNITS[u][1]
        return (0, 512) if b is None else (b * 256, 256)

    def halves(u):
        b = UNITS[u][1]
        return (0, 1) if b is None else (b,)

    def products(low, size, u):
        j, b = UNITS[u]
        cols = slice(0, 256) if b is None else slice(b * 128, b * 128 + 128)
        parts = []
        for a in (0, 1):
            part = jnp.dot(ag[a, low : low + size, :], wg[a, j, :, cols], preferred_element_type=F32)
            parts.append({v: part[:, i * 128 : i * 128 + 128] for i, v in enumerate(halves(u))})
        return parts

    def first(u, group):
        low, size = group
        j = UNITS[u][0]
        need_w(u)
        if group != OWN:
            need_rows(0, group)
        parts = products(low, size, u)
        copies = []
        for a in (0, 1):
            for b in halves(u):
                at = b * 256 + a * 128
                ring_out[a, 0, j, low : low + size, at : at + 128] = parts[a][b].astype(BF16)
                rows, cols = pl.ds(low, size), pl.ds(at, 128)
                copies.append(send(
                    ring_out.at[a, 0, j, rows, cols], ring_in.at[a, 0, j, rows, cols],
                    f_send, f_recv.at[u, int(group == FAR)], **{"head": sides[a]},
                ))
        start(copies)

    def ring_wait(stage, u, group):
        low, size = group
        n = unit_cols(u)[1]
        sem = (f_recv.at[u, int(group == FAR)] if stage == 0 else r_recv.at[stage - 1, u, int(group == FAR)])
        if stage == 0:
            all_of(ring_in.at[0, 0, 0, pl.ds(low, size), pl.ds(0, n)], sem)
        else:
            all_of(ring_in.at[0, 0, pl.ds(0, 2), pl.ds(low, size), pl.ds(0, n)], sem)

    def middle(stage, u, group=ALL):
        p = 2 * stage - 1
        low, size = group
        j = UNITS[u][0]
        need_w(u)
        need_rows(p, group)
        need_rows(p + 1, group)
        if group == ALL:
            both = products(p * 128, 256, u)
            parts = [[{b: both[a][b][side * 128 : side * 128 + 128] for b in halves(u)} for a in (0, 1)] for side in (0, 1)]
        else:
            parts = [products((p + side) * 128 + low, size, u) for side in (0, 1)]
        for waited in ((NEAR, FAR) if group == ALL and split(stage - 1, u) else (group,)):
            ring_wait(stage - 1, u, waited)
        rows = slice(low, low + size)
        for side in (0, 1):
            for b in halves(u):
                for a in (0, 1):
                    cols = slice(b * 256 + a * 128, b * 256 + a * 128 + 128)
                    got = ring_in[side, stage - 1, j, rows, cols].astype(F32)
                    ring_out[side, stage, j, rows, cols] = (parts[side][a][b] + got).astype(BF16)
        at = (pl.ds(low, size), pl.ds(*unit_cols(u)))
        start([
            send(
                ring_out.at[(side, stage, j, *at)], ring_in.at[(side, stage, j, *at)],
                r_send, r_recv.at[stage - 1, u, int(group == FAR)], **{"head": sides[side]},
            )
            for side in (0, 1)
        ])

    def split(stage, u):
        return u < SPLIT_UNITS and stage <= SPLIT

    def final(u):
        j, b = UNITS[u]
        need_w(u)
        need_rows(7, ALL)
        parts = products(896, 128, u)
        for waited in ((NEAR, FAR) if split(3, u) else (ALL,)):
            ring_wait(3, u, waited)
        low, n = (0, 256) if b is None else (b * 128, 128)
        copies = []
        for a in (0, 1):
            for v in halves(u):
                at = v * 256 + a * 128
                total = parts[a][v] + ring_in[0, 3, j, :, at : at + 128].astype(F32) + ring_in[1, 3, j, :, at : at + 128].astype(F32)
                done[a, j, :, v * 128 : v * 128 + 128] = total.astype(BF16)
            shard = ring_at[0][j] * 4 + y if a == 0 else x * 4 + ring_at[1][j]
            cols = pl.ds(pl.multiple_of(shard * 512 + a * 256 + low, 128), n)
            for r in (3, 1, 2, 0):
                axis = {SEQ[1 - a]: ring_at[1 - a][r]}
                copies.append(send(
                    done.at[a, j, pl.ds(r * 32, 32), pl.ds(low, n)], out.at[:, cols], o_sem.at[0], o_sem.at[1], section=1 - s, **axis
                ))
        start(copies)

    for op, *at in ORDER:
        if op == "hd":
            hidden(*at)
            start(direct[at[0]])
        if op == "fw":
            need(("direct", *at))
            start(passed[at[0]])
        if op == "wf":
            need(("w", *at))
            start(w_forward(*at))
        if op == "wb":
            start(w_direct(1, 0, 1024, (w_send, w_recv.at[1])))
        if op == "first":
            first(*at)
        if op == "mid":
            middle(*at)
        if op == "fin":
            final(*at)

    all_of(decay.at[pl.ds(0, 15)], d_sem.at[0])
    all_of(state.at[pl.ds(0, 240)], s_sem.at[0])
    all_of(state.at[pl.ds(0, 240)], t_sem.at[0])
    all_of(ag.at[0], w_send)
    all_of(ag.at[0, pl.ds(0, 512)], wf_send)
    all_of(ag.at[0, pl.ds(0, 256)], f_send)
    all_of(ag.at[0], a_send.at[0])
    all_of(ag.at[0, pl.ds(0, 512)], a_send.at[1])
    all_of(ring_out.at[:, pl.ds(1, 3)], r_send)
    all_of(done, o_sem.at[0])

    @pl.when(q < 15)
    def _():
        for c in halo:
            c.wait_send()

    all_of(out, o_sem.at[1])


def per_device(
    x_in, b_in, c_in, z_in, dt_raw, conv_x, conv_b, conv_c, a_rate, dt_bias, skip_d, norm_gain, out_weight
):
    dma = pltpu.SemaphoreType.DMA
    half = lambda *shape: pltpu.VMEM(shape, BF16)
    full = lambda *shape: pltpu.VMEM(shape, F32)
    anywhere = pl.BlockSpec(memory_space=pl.ANY)
    mixed = pl.pallas_call(
        mixer_kernel,
        out_shape=pltpu.VMEM((32, 8192), BF16),
        in_specs=[anywhere] * 13,
        out_specs=pl.BlockSpec(memory_space=pltpu.VMEM),
        scratch_shapes=[
            half(256, 1024), half(256, 256), half(256, 256), half(256, 1024), full(16, 256),
            full(4, 1024), full(4, 256), full(4, 256), full(1, 16), full(1, 16), full(1, 16), full(1, 1024),
            half(16, 1024), half(16, 256), half(16, 256), full(264, 1024), full(264, 256), full(264, 256),
            half(256, 1024), half(256, 256), half(256, 256), half(256, 1024),
            full(16, 256), full(16, 256), full(8, 128), full(16, 8, 128),
            half(256, 1024), half(16, 16, 1024), half(16, 16, 1024), half(256, 1024),
            full(256, 256), full(256, 1024), full(256, 1024), full(256, 1024),
            half(2, 4, 1024, 256), half(2, 1024, 1024), half(2, 4, 4, 128, 512), half(2, 4, 4, 128, 512), half(2, 4, 128, 256),
            dma((12,)), dma((3,)), dma((3,)), dma((2,)), dma((2,)), dma((2,)),
            dma((2,)), dma, dma((2,)), dma, dma((2,)), dma, dma((7, 2)), dma((2,)), dma((2, 8)), dma, dma((3, 7, 2)), dma((2,)),
        ],
        compiler_params=pltpu.CompilerParams(
            collective_id=0, has_side_effects=True, vmem_limit_bytes=56 * 2**20
        ),
    )(
        x_in[0], b_in[0], c_in[0], z_in[0], dt_raw[0], conv_x[0], conv_b[0], conv_c[0],
        a_rate, dt_bias, skip_d, norm_gain, out_weight[0],
    )
    return mixed[None]


def solution(mesh):
    finer = Mesh(
        mesh.devices.reshape(mesh.shape["section"], 4, 4, mesh.shape["head"]),
        ("section", "seq_0", "seq_1", "head"),
    )
    return jax.shard_map(
        per_device,
        mesh=finer,
        in_specs=(
            P("section", SEQ, "head"),
            P("section", SEQ, "head"),
            P("section", SEQ, "head"),
            P("section", SEQ, "head"),
            P("section", "head", SEQ),
            P("section", None, "head"),
            P("section", None, "head"),
            P("section", None, "head"),
            P("section", "head"),
            P("section", "head"),
            P("section", "head"),
            P("section", "head"),
            P("section", "head", SEQ),
        ),
        out_specs=P("section", SEQ_HEAD, None),
        check_vma=False,
    )
```

```python
import jax
import jax.numpy as jnp
from jax import lax
from jax.experimental import pallas as pl
from jax.experimental.pallas import tpu as pltpu
from jax.sharding import Mesh
from jax.sharding import PartitionSpec as P

SEQ = ("seq_0", "seq_1")
SEQ_HEAD = ("seq_0", "seq_1", "head")
MESH = pl.DeviceIdType.MESH
PIECES = (4, 3, 5, 2, 6, 1, 7, 0)
OFFSETS = (0, 3, 1, 2)
PEERS = tuple((dx, dy) for dx in (2, 1, 3, 0) for dy in (2, 1, 3, 0) if dx or dy)
W_CUT = 672
UNITS = ((0, None), (1, 0), (2, 0), (1, 1), (2, 1), (3, 0), (3, 1))
ALL, FAR, OWN, SIDE = (0, 128), (96, 32), (0, 32), (32, 64)
SLOT = {ALL: 0, OWN: 0, SIDE: 1, FAR: 2}
F32 = jnp.float32
ORDER = (
    ("hd", 0), ("first", 1, OWN), ("hd", 4), ("first", 2, OWN), ("hd", 2), ("hd", 1),
    ("first", 0, OWN), ("mid", 1, 1, OWN), ("fw", 0), ("wb",), ("mid", 1, 2, OWN), ("mid", 1, 0, OWN),
    ("first", 1, SIDE), ("hd", 3), ("first", 2, SIDE), ("first", 0, SIDE), ("mid", 2, 1, OWN), ("mid", 2, 2, OWN),
    ("mid", 2, 0, OWN), ("fw", 1), ("mid", 1, 1, SIDE), ("first", 1, FAR), ("mid", 1, 0, SIDE), ("mid", 1, 2, SIDE),
    ("first", 0, FAR), ("first", 2, FAR), ("fw", 2), ("hd", 5), ("hd", 6), ("mid", 3, 2, OWN),
    ("mid", 3, 1, OWN), ("mid", 3, 0, OWN), ("wf", 0), ("first", 4, ALL), ("first", 3, ALL), ("wf", 1),
    ("mid", 2, 0, SIDE), ("mid", 2, 2, SIDE), ("mid", 1, 2, FAR), ("mid", 2, 1, SIDE), ("fw", 4), ("mid", 1, 0, FAR),
    ("fw", 3), ("mid", 1, 3, ALL), ("mid", 1, 4, ALL), ("mid", 1, 1, FAR), ("first", 5, ALL), ("mid", 3, 0, SIDE),
    ("fw", 5), ("mid", 3, 1, SIDE), ("first", 6, ALL), ("mid", 3, 2, SIDE), ("fw", 6), ("mid", 2, 0, FAR),
    ("mid", 2, 2, FAR), ("mid", 2, 1, FAR), ("mid", 1, 5, ALL), ("mid", 1, 6, ALL), ("mid", 2, 3, ALL), ("hd", 7),
    ("mid", 2, 4, ALL), ("mid", 2, 5, ALL), ("mid", 2, 6, ALL), ("mid", 3, 2, FAR), ("mid", 3, 1, FAR), ("fw", 7),
    ("mid", 3, 0, FAR), ("mid", 3, 3, SIDE), ("mid", 3, 4, FAR), ("mid", 3, 3, FAR), ("mid", 3, 5, ALL), ("mid", 3, 6, FAR),
    ("mid", 3, 4, SIDE), ("mid", 3, 6, SIDE), ("fin", 0, ALL), ("fin", 2, ALL), ("mid", 3, 6, OWN), ("mid", 3, 4, OWN),
    ("mid", 3, 3, OWN), ("fin", 4, FAR), ("fin", 1, ALL), ("fin", 5, ALL), ("fin", 3, FAR), ("fin", 6, FAR),
    ("fin", 3, SIDE), ("fin", 4, SIDE), ("fin", 6, SIDE), ("fin", 6, OWN), ("fin", 4, OWN), ("fin", 3, OWN),
)
BF16 = jnp.bfloat16

SPLIT = 3
SPLIT_UNITS = 3
TAILS = (3, 4, 6)
epsilon = 1e-05


def send(src, dst, send_sem, recv_sem, **to):
    return pltpu.make_async_remote_copy(
        src_ref=src, dst_ref=dst, send_sem=send_sem, recv_sem=recv_sem,
        device_id=to, device_id_type=MESH,
    )


def exact_dot(a, b):
    return jnp.dot(a, b, precision=lax.Precision.HIGHEST, preferred_element_type=F32)


def conv_blocks(padded, kernel, out, blocks):
    def columns(i, _):
        cols = pl.ds(pl.multiple_of(i * 256, 256), 256)
        for block in blocks:
            summed = jnp.zeros((64, 256), F32)
            for k in range(4):
                summed = summed + kernel[k : k + 1, cols] * padded[block * 64 + 5 + k : block * 64 + 69 + k, cols]
            out[block * 64 : block * 64 + 64, cols] = (summed * jax.nn.sigmoid(summed)).astype(BF16)
        return 0

    lax.fori_loop(0, out.shape[1] // 256, columns, 0)


def mixer_kernel(
    x_hbm, b_hbm, c_hbm, z_hbm, dt_hbm, conv_x_hbm, conv_b_hbm, conv_c_hbm, rate_hbm, bias_hbm, skip_hbm, gain_hbm, w, out,
    x_in, b_in, c_in, z_in, dt, conv_x, conv_b, conv_c, rate, bias, skip, gain,
    halo_x, halo_b, halo_c, pad_x, pad_b, pad_c, xc, bc, cc, xw,
    step, logd, decay_own, decay, state, state_in, state_out, carried, scores, inside, grow, to_end,
    wg, ag, ring_out, ring_in, done,
    l_sem, h_send, h_recv, d_sem, s_sem, t_sem,
    w_own, w_send, w_recv, wf_send, wf_recv, f_send, f_recv, a_send, a_recv, r_send, r_recv, o_sem,
):
    s, x, y, h = (lax.axis_index(a) for a in ("section", "seq_0", "seq_1", "head"))
    q = x * 4 + y
    ring_at = [[lax.rem(v + o, 4) for o in OFFSETS] for v in (x, y)]
    sides = (lax.rem(h + 1, 8), lax.rem(h + 7, 8))
    peers = [(lax.rem(x + dx, 4), lax.rem(y + dy, 4)) for dx, dy in PEERS]

    barrier = pltpu.get_barrier_semaphore()
    greeted = (
        [{"seq_0": u, "seq_1": v} for u, v in peers]
        + [{"head": v} for v in sides]
        + [{"section": 1 - s, "seq_1": v} for v in ring_at[1]]
        + [{"section": 1 - s, "seq_0": v} for v in ring_at[0][1:]]
    )
    for peer in greeted:
        pl.semaphore_signal(barrier, inc=1, device_id=peer, device_id_type=MESH)

    loads = {}
    for i, (name, src, dst) in enumerate((
        ("dt", dt_hbm, dt), ("bias", bias_hbm, bias), ("rate", rate_hbm, rate),
        ("b", b_hbm, b_in), ("x", x_hbm, x_in), ("c", c_hbm, c_in),
        ("kb", conv_b_hbm, conv_b), ("kx", conv_x_hbm, conv_x), ("kc", conv_c_hbm, conv_c),
        ("skip", skip_hbm, skip), ("z", z_hbm, z_in), ("gain", gain_hbm, gain),
    )):
        loads[name] = pltpu.make_async_copy(src, dst, l_sem.at[i])
        loads[name].start()
    own_w = [pltpu.make_async_copy(w.at[:, pl.ds(a * 256, 256)], wg.at[a, 0], w_own.at[a]) for a in (0, 1)]
    for c in own_w:
        c.start()

    def loaded(*names):
        for n in names:
            loads[n].wait()

    def all_of(ref, sem):
        pltpu.make_async_copy(ref, ref, sem).wait()

    def start(copies):
        for c in copies:
            c.start()

    loaded("b", "x", "c")
    pl.semaphore_wait(barrier, len(greeted))

    to_next = {"seq_0": lax.rem(x + lax.div(y + 1, 4), 4), "seq_1": lax.rem(y + 1, 4)}
    halo = [
        send(src.at[pl.ds(240, 16)], dst, h_send.at[i], h_recv.at[i], **to_next)
        for i, (src, dst) in enumerate(((b_in, halo_b), (x_in, halo_x), (c_in, halo_c)))
    ]

    @pl.when(q < 15)
    def _():
        for c in halo:
            c.start()

    def w_direct(b, low, size, sems):
        rows = pl.ds(low, size)
        copies = []
        for a in (0, 1):
            for slot, to in ((1, 2), (2, 1)):
                copies.append(send(
                    w.at[rows, pl.ds(a * 256 + b * 128, 128)], wg.at[a, slot, rows, pl.ds(b * 128, 128)],
                    sems[0], sems[1], **{SEQ[a]: ring_at[a][to]},
                ))
        return copies

    start(w_direct(0, 0, W_CUT, (w_send, w_recv.at[0])))
    loaded("dt", "bias", "rate")
    row16 = lax.broadcasted_iota(jnp.int32, (16, 16), 0)
    col16 = lax.broadcasted_iota(jnp.int32, (16, 16), 1)

    def column(row):
        return jnp.sum(jnp.where(row16 == col16, jnp.broadcast_to(row, (16, 16)), 0.0), axis=1, keepdims=True)

    raw = dt[...] + column(bias[...])
    step_size = jnp.maximum(raw, 0.0) + jnp.log1p(jnp.exp(-jnp.abs(raw)))
    log_decay = -column(rate[...]) * step_size
    lane = lax.broadcasted_iota(jnp.int32, (16, 256), 1)
    for shift in (1, 2, 4, 8, 16, 32, 64, 128):
        log_decay = log_decay + jnp.where(lane >= shift, pltpu.roll(log_decay, shift, 1), 0.0)
    step[...] = step_size
    logd[...] = log_decay
    spread = jnp.where(
        lax.shift_right_logical(lax.broadcasted_iota(jnp.int32, (16, 1024), 1), 6)
        == lax.broadcasted_iota(jnp.int32, (16, 1024), 0), 1.0, 0.0,
    ).astype(F32)
    log_cols = log_decay.T
    end_cols = (jnp.exp(log_decay[:, 255:256] - log_decay) * step_size).T
    last = exact_dot(jnp.exp(log_cols[248:256, :]), spread)[7:8, :]
    for r in range(8):
        decay_own[r : r + 1, :] = last[:, r * 128 : r * 128 + 128]
    decay[q] = decay_own[...]

    start([
        send(decay_own, decay.at[q], d_sem.at[0], d_sem.at[1], seq_0=u, seq_1=v)
        for i, (u, v) in enumerate(peers)
    ])

    loaded("kb", "kx", "kc", "skip", "z", "gain")
    pad_x[8:264, :] = x_in[...].astype(F32)
    pad_b[8:264, :] = b_in[...].astype(F32)
    pad_c[8:264, :] = c_in[...].astype(F32)
    to_end[...] = exact_dot(end_cols, spread)
    conv_blocks(pad_b, conv_b, bc, (1, 2, 3))
    conv_blocks(pad_x, conv_x, xc, (1, 2, 3))

    def finish(i, halo_ref, padded, kernel, conv_out):
        @pl.when(q > 0)
        def _():
            halo[i].wait_recv()
            padded[0:8, :] = halo_ref[...].astype(F32)[8:16]

        @pl.when(q == 0)
        def _():
            padded[0:8, :] = jnp.zeros((8, padded.shape[1]), F32)

        conv_blocks(padded, kernel, conv_out, (0,))

    finish(0, halo_b, pad_b, conv_b, bc)
    finish(1, halo_x, pad_x, conv_x, xc)

    b_cols = bc[...].astype(F32).T.astype(BF16)
    for i in range(4):
        cols = slice(i * 256, i * 256 + 256)
        xw[:, cols] = (xc[:, cols].astype(F32) * to_end[:, cols]).astype(BF16)
        state[:, cols] = jnp.dot(b_cols, xw[:, cols], preferred_element_type=F32).astype(BF16)
    state_in[q] = state[pl.ds(pl.multiple_of(q * 16, 16), 16), :]
    start([
        send(
            state.at[pl.ds(pl.multiple_of((u * 4 + v) * 16, 16), 16)], state_in.at[q],
            s_sem.at[0], s_sem.at[1], seq_0=u, seq_1=v,
        )
        for i, (u, v) in enumerate(peers)
    ])
    start(w_direct(0, W_CUT, 1024 - W_CUT, (w_send, w_recv.at[0])))

    conv_blocks(pad_c, conv_c, cc, (1, 2, 3))
    finish(2, halo_c, pad_c, conv_c, cc)
    scores[...] = lax.dot_general(cc[...], bc[...], (((1,), (1,)), ((), ())), preferred_element_type=F32)
    skip_row = exact_dot(jnp.broadcast_to(skip[...], (8, 16)), spread)[0:1, :]
    causal = lax.broadcasted_iota(jnp.int32, (128, 128), 0) >= lax.broadcasted_iota(jnp.int32, (128, 128), 1)
    first_half = lax.broadcasted_iota(jnp.int32, (256, 128), 1) < 64
    grow_cols = jnp.exp(log_cols)

    def damped(log_col, head, rows, cols, masked):
        value = jnp.exp(jnp.minimum(log_col[rows] - logd[head : head + 1, cols], 0.0))
        if masked:
            value = jnp.where(causal, value, 0.0)
        return (value * step[head : head + 1, cols] * scores[rows, cols]).astype(BF16)

    top, bottom = slice(0, 128), slice(128, 256)

    def pair(g):
        lanes = slice(g * 128, g * 128 + 128)
        parts = []
        for head in (2 * g, 2 * g + 1):
            log_col = log_cols[:, head : head + 1]
            upper = jnp.dot(damped(log_col, head, top, top, True), xc[top, lanes], preferred_element_type=F32)
            lower = jnp.dot(damped(log_col, head, bottom, top, False), xc[top, lanes], preferred_element_type=F32)
            lower = lower + jnp.dot(damped(log_col, head, bottom, bottom, True), xc[bottom, lanes], preferred_element_type=F32)
            parts.append(jnp.concatenate([upper, lower], axis=0))
        both = jnp.where(first_half, parts[0], parts[1])
        zf = z_in[:, lanes].astype(F32)
        gate = zf * jax.nn.sigmoid(zf)
        inside[:, lanes] = (both + skip_row[:, lanes] * xc[:, lanes].astype(F32)) * gate
        grow[:, lanes] = exact_dot(grow_cols, spread[:, lanes]) * gate

    for g in range(4):
        pair(g)

    all_of(decay.at[pl.ds(0, 15)], d_sem.at[1])
    all_of(state.at[pl.ds(0, 240)], s_sem.at[1])
    for r in range(8):
        lanes = slice(r * 128, r * 128 + 128)
        acc = jnp.zeros((16, 128), F32)
        for k in range(16):
            state_out[k, :, lanes] = acc.astype(BF16)
            if k < 15:
                acc = decay[k, r : r + 1, :] * acc + state_in[k, :, lanes].astype(F32)
    my_rows = pl.ds(pl.multiple_of(q * 16, 16), 16)
    start([
        send(state_out.at[u * 4 + v], carried.at[my_rows], t_sem.at[0], t_sem.at[1], seq_0=u, seq_1=v)
        for i, (u, v) in enumerate(peers)
    ])
    carried[my_rows, :] = state_out[q]

    def w_forward(b):
        cols = pl.ds(b * 128, 128)
        copies = []
        for a in (0, 1):
            for slot, to, low in ((1, 2, 0), (2, 1, 512)):
                at = (pl.ds(low, 512), cols)
                copies.append(send(
                    wg.at[(a, slot, *at)], wg.at[(a, 3, *at)], wf_send, wf_recv.at[b], **{SEQ[a]: ring_at[a][to]},
                ))
        return copies

    for g in range(4, 8):
        pair(g)
    for side in (0, 1):
        for j in range(4):
            for b in (0, 1):
                at = b * 256 + (1 - side) * 128
                ring_in[side, 0, j, :, at : at + 128] = jnp.zeros((128, 128), BF16)
    def a_direct(p):
        copies = []
        for a in (0, 1):
            mine, all_rows = ag.at[a, pl.ds(p * 128, 32)], ag.at[a]
            axis, to = SEQ[1 - a], ring_at[1 - a]
            copies += [
                send(mine, all_rows.at[pl.ds(p * 128 + 32, 32)], a_send.at[0], a_recv.at[0, p], **{axis: to[2]}),
                send(mine, all_rows.at[pl.ds(p * 128 + 64, 32)], a_send.at[0], a_recv.at[0, p], **{axis: to[1]}),
            ]
        return copies

    def a_forward(p):
        copies = []
        for a in (0, 1):
            rows = ag.at[a]
            axis, to = SEQ[1 - a], ring_at[1 - a]
            copies += [
                send(rows.at[pl.ds(p * 128 + 32, 16)], rows.at[pl.ds(p * 128 + 96, 16)], a_send.at[1], a_recv.at[1, p], **{axis: to[2]}),
                send(rows.at[pl.ds(p * 128 + 80, 16)], rows.at[pl.ds(p * 128 + 112, 16)], a_send.at[1], a_recv.at[1, p], **{axis: to[1]}),
            ]
        return copies

    direct = {p: a_direct(p) for p in range(8)}
    passed = {p: a_forward(p) for p in range(8)}

    all_of(state.at[pl.ds(0, 240)], t_sem.at[1])

    def hidden(p):
        rows = pl.ds(pl.multiple_of(lax.rem(h + PIECES[p], 8) * 32, 32), 32)
        outside = jnp.dot(cc[rows, :], carried[...], preferred_element_type=F32)
        gated = inside[rows, :] + outside * grow[rows, :]
        inverse_rms = lax.rsqrt(jnp.mean(gated * gated, axis=1, keepdims=True) + epsilon)
        value = (gated * inverse_rms * gain[...]).astype(BF16)
        ag[0, p * 128 : p * 128 + 32, :] = value
        ag[1, p * 128 : p * 128 + 32, :] = value

    seen, ring_seen = set(), set()

    def need(key):
        if key in seen:
            return
        seen.add(key)
        kind, index = key
        if kind == "own":
            for c in own_w:
                c.wait()
        if kind == "direct":
            all_of(ag.at[0, pl.ds(0, 128)], a_recv.at[0, index])
        if kind == "passed":
            all_of(ag.at[0, pl.ds(0, 64)], a_recv.at[1, index])
        if kind == "w":
            all_of(ag.at[0, pl.ds(0, 512)], w_recv.at[index])
        if kind == "wf":
            all_of(ag.at[0, pl.ds(0, 256)], wf_recv.at[index])

    def need_rows(p, group):
        if group != OWN:
            need(("direct", p))
        if group in (ALL, FAR):
            need(("passed", p))

    def need_w(u):
        j, b = UNITS[u]
        need(("own", 0))
        if j in (1, 2):
            need(("w", b))
        if j == 3:
            need(("wf", b))

    def unit_cols(u):
        b = UNITS[u][1]
        return (0, 512) if b is None else (b * 256, 256)

    def halves(u):
        b = UNITS[u][1]
        return (0, 1) if b is None else (b,)

    def products(low, size, u):
        j, b = UNITS[u]
        cols = slice(0, 256) if b is None else slice(b * 128, b * 128 + 128)
        parts = []
        for a in (0, 1):
            part = jnp.dot(ag[a, low : low + size, :], wg[a, j, :, cols], preferred_element_type=F32)
            parts.append({v: part[:, i * 128 : i * 128 + 128] for i, v in enumerate(halves(u))})
        return parts

    def first(u, group):
        low, size = group
        j = UNITS[u][0]
        need_w(u)
        if group != OWN:
            need_rows(0, group)
        parts = products(low, size, u)
        copies = []
        for a in (0, 1):
            for b in halves(u):
                at = b * 256 + a * 128
                ring_out[a, 0, j, low : low + size, at : at + 128] = parts[a][b].astype(BF16)
                rows, cols = pl.ds(low, size), pl.ds(at, 128)
                copies.append(send(
                    ring_out.at[a, 0, j, rows, cols], ring_in.at[a, 0, j, rows, cols],
                    f_send, f_recv.at[u, SLOT[group]], **{"head": sides[a]},
                ))
        start(copies)

    def ring_need(stage, u, group):
        groups = (OWN, SIDE, FAR) if split(stage, u) else (ALL,)
        for waited in groups:
            if group in (ALL, waited) or waited == ALL:
                if (stage, u, waited) not in ring_seen:
                    ring_seen.add((stage, u, waited))
                    ring_wait(stage, u, waited)

    def ring_wait(stage, u, group):
        low, size = group
        n = unit_cols(u)[1]
        sem = (f_recv.at[u, SLOT[group]] if stage == 0 else r_recv.at[stage - 1, u, SLOT[group]])
        if stage == 0:
            all_of(ring_in.at[0, 0, 0, pl.ds(low, size), pl.ds(0, n)], sem)
        else:
            all_of(ring_in.at[0, 0, pl.ds(0, 2), pl.ds(low, size), pl.ds(0, n)], sem)

    def middle(stage, u, group=ALL):
        p = 2 * stage - 1
        low, size = group
        j = UNITS[u][0]
        need_w(u)
        need_rows(p, group)
        need_rows(p + 1, group)
        if group == ALL:
            both = products(p * 128, 256, u)
            parts = [[{b: both[a][b][side * 128 : side * 128 + 128] for b in halves(u)} for a in (0, 1)] for side in (0, 1)]
        else:
            parts = [products((p + side) * 128 + low, size, u) for side in (0, 1)]
        ring_need(stage - 1, u, group)
        rows = slice(low, low + size)
        for side in (0, 1):
            for b in halves(u):
                for a in (0, 1):
                    cols = slice(b * 256 + a * 128, b * 256 + a * 128 + 128)
                    got = ring_in[side, stage - 1, j, rows, cols].astype(F32)
                    ring_out[side, stage, j, rows, cols] = (parts[side][a][b] + got).astype(BF16)
        at = (pl.ds(low, size), pl.ds(*unit_cols(u)))
        start([
            send(
                ring_out.at[(side, stage, j, *at)], ring_in.at[(side, stage, j, *at)],
                r_send, r_recv.at[stage - 1, u, SLOT[group]], **{"head": sides[side]},
            )
            for side in (0, 1)
        ])

    def split(stage, u):
        return (u < SPLIT_UNITS and stage <= SPLIT) or (u in TAILS and stage == 3)

    def final(u, group):
        j, b = UNITS[u]
        first_row, size = group
        rows = slice(first_row, first_row + size)
        need_w(u)
        need_rows(7, group)
        parts = products(896 + first_row, size, u)
        ring_need(3, u, group)
        low, n = (0, 256) if b is None else (b * 128, 128)
        copies = []
        for a in (0, 1):
            for v in halves(u):
                at = v * 256 + a * 128
                total = parts[a][v]
                for side in (0, 1):
                    total = total + ring_in[side, 3, j, rows, at : at + 128].astype(F32)
                done[a, j, rows, v * 128 : v * 128 + 128] = total.astype(BF16)
            shard = ring_at[0][j] * 4 + y if a == 0 else x * 4 + ring_at[1][j]
            cols = pl.ds(pl.multiple_of(shard * 512 + a * 256 + low, 128), n)
            for r in (3, 1, 2, 0):
                if first_row <= r * 32 < first_row + size:
                    axis = {SEQ[1 - a]: ring_at[1 - a][r]}
                    copies.append(send(
                        done.at[a, j, pl.ds(r * 32, 32), pl.ds(low, n)], out.at[:, cols], o_sem.at[0], o_sem.at[1], section=1 - s, **axis
                    ))
        start(copies)

    for op, *at in ORDER:
        if op == "hd":
            hidden(*at)
            start(direct[at[0]])
        if op == "fw":
            need(("direct", *at))
            start(passed[at[0]])
        if op == "wf":
            need(("w", *at))
            start(w_forward(*at))
        if op == "wb":
            start(w_direct(1, 0, 1024, (w_send, w_recv.at[1])))
        if op == "first":
            first(*at)
        if op == "mid":
            middle(*at)
        if op == "fin":
            final(*at)

    all_of(decay.at[pl.ds(0, 15)], d_sem.at[0])
    all_of(state.at[pl.ds(0, 240)], s_sem.at[0])
    all_of(state.at[pl.ds(0, 240)], t_sem.at[0])
    all_of(ag.at[0], w_send)
    all_of(ag.at[0, pl.ds(0, 512)], wf_send)
    all_of(ag.at[0, pl.ds(0, 256)], f_send)
    all_of(ag.at[0], a_send.at[0])
    all_of(ag.at[0, pl.ds(0, 512)], a_send.at[1])
    all_of(ring_out.at[:, pl.ds(1, 3)], r_send)
    all_of(done, o_sem.at[0])

    @pl.when(q < 15)
    def _():
        for c in halo:
            c.wait_send()

    all_of(out, o_sem.at[1])


def per_device(
    x_in, b_in, c_in, z_in, dt_raw, conv_x, conv_b, conv_c, a_rate, dt_bias, skip_d, norm_gain, out_weight
):
    dma = pltpu.SemaphoreType.DMA
    half = lambda *shape: pltpu.VMEM(shape, BF16)
    full = lambda *shape: pltpu.VMEM(shape, F32)
    anywhere = pl.BlockSpec(memory_space=pl.ANY)
    mixed = pl.pallas_call(
        mixer_kernel,
        out_shape=pltpu.VMEM((32, 8192), BF16),
        in_specs=[anywhere] * 13,
        out_specs=pl.BlockSpec(memory_space=pltpu.VMEM),
        scratch_shapes=[
            half(256, 1024), half(256, 256), half(256, 256), half(256, 1024), full(16, 256),
            full(4, 1024), full(4, 256), full(4, 256), full(1, 16), full(1, 16), full(1, 16), full(1, 1024),
            half(16, 1024), half(16, 256), half(16, 256), full(264, 1024), full(264, 256), full(264, 256),
            half(256, 1024), half(256, 256), half(256, 256), half(256, 1024),
            full(16, 256), full(16, 256), full(8, 128), full(16, 8, 128),
            half(256, 1024), half(16, 16, 1024), half(16, 16, 1024), half(256, 1024),
            full(256, 256), full(256, 1024), full(256, 1024), full(256, 1024),
            half(2, 4, 1024, 256), half(2, 1024, 1024), half(2, 4, 4, 128, 512), half(2, 4, 4, 128, 512), half(2, 4, 128, 256),
            dma((12,)), dma((3,)), dma((3,)), dma((2,)), dma((2,)), dma((2,)),
            dma((2,)), dma, dma((2,)), dma, dma((2,)), dma, dma((7, 3)), dma((2,)), dma((2, 8)), dma, dma((3, 7, 3)), dma((2,)),
        ],
        compiler_params=pltpu.CompilerParams(
            collective_id=0, has_side_effects=True, vmem_limit_bytes=56 * 2**20
        ),
    )(
        x_in[0], b_in[0], c_in[0], z_in[0], dt_raw[0], conv_x[0], conv_b[0], conv_c[0],
        a_rate, dt_bias, skip_d, norm_gain, out_weight[0],
    )
    return mixed[None]


def solution(mesh):
    finer = Mesh(
        mesh.devices.reshape(mesh.shape["section"], 4, 4, mesh.shape["head"]),
        ("section", "seq_0", "seq_1", "head"),
    )
    return jax.shard_map(
        per_device,
        mesh=finer,
        in_specs=(
            P("section", SEQ, "head"),
            P("section", SEQ, "head"),
            P("section", SEQ, "head"),
            P("section", SEQ, "head"),
            P("section", "head", SEQ),
            P("section", None, "head"),
            P("section", None, "head"),
            P("section", None, "head"),
            P("section", "head"),
            P("section", "head"),
            P("section", "head"),
            P("section", "head"),
            P("section", "head", SEQ),
        ),
        out_specs=P("section", SEQ_HEAD, None),
        check_vma=False,
    )
```

```python
import jax
import jax.numpy as jnp
from jax import lax
from jax.experimental import pallas as pl
from jax.experimental.pallas import tpu as pltpu
from jax.sharding import Mesh
from jax.sharding import PartitionSpec as P

SEQ = ("seq_0", "seq_1")
SEQ_HEAD = ("seq_0", "seq_1", "head")
MESH = pl.DeviceIdType.MESH
PIECES = (4, 3, 5, 2, 6, 1, 7, 0)
OFFSETS = (0, 3, 1, 2)
PEERS = (
    (2, 2), (1, 2), (3, 2), (2, 1), (2, 3), (0, 2), (2, 0), (1, 1), (3, 3), (1, 3), (3, 1), (0, 1), (3, 0), (0, 3), (1, 0),
)
W_CUT = 672
UNITS = ((0, None), (1, 0), (2, 0), (1, 1), (2, 1), (3, 0), (3, 1))
ALL, FAR, OWN, SIDE = (0, 128), (96, 32), (0, 32), (32, 64)
SLOT = {ALL: 0, OWN: 0, SIDE: 1, FAR: 2}
F32 = jnp.float32
ORDER = (
    ("wb", 2), ("hd", 0), ("first", 2, OWN), ("hd", 1), ("first", 0, OWN), ("hd", 2),
    ("first", 1, OWN), ("wb", 0), ("mid", 1, 2, OWN), ("mid", 1, 0, OWN), ("mid", 1, 1, OWN), ("first", 0, SIDE),
    ("first", 1, SIDE), ("fw", 0), ("wb", 3), ("wb", 1), ("hd", 4), ("hd", 3),
    ("first", 2, SIDE), ("mid", 2, 2, OWN), ("mid", 2, 0, OWN), ("mid", 2, 1, OWN), ("fw", 1), ("fw", 2),
    ("mid", 1, 0, SIDE), ("wf", 0), ("mid", 1, 1, SIDE), ("hd", 6), ("hd", 5), ("first", 2, FAR),
    ("first", 1, FAR), ("mid", 3, 2, OWN), ("mid", 1, 2, SIDE), ("mid", 3, 0, OWN), ("first", 4, ALL), ("first", 3, ALL),
    ("mid", 3, 1, OWN), ("wf", 1), ("first", 0, FAR), ("mid", 2, 0, SIDE), ("fw", 4), ("mid", 2, 1, SIDE),
    ("fw", 3), ("mid", 2, 2, SIDE), ("mid", 1, 4, ALL), ("mid", 1, 1, FAR), ("first", 5, ALL), ("mid", 1, 0, FAR),
    ("mid", 1, 3, ALL), ("mid", 3, 2, SIDE), ("mid", 3, 0, SIDE), ("hd", 7), ("fw", 5), ("mid", 1, 2, FAR),
    ("first", 6, ALL), ("fw", 6), ("mid", 1, 5, ALL), ("mid", 2, 4, ALL), ("mid", 2, 1, FAR), ("mid", 2, 0, FAR),
    ("mid", 2, 2, FAR), ("mid", 1, 6, ALL), ("mid", 2, 5, ALL), ("mid", 2, 3, ALL), ("mid", 3, 4, FAR), ("fw", 7),
    ("mid", 3, 2, FAR), ("mid", 3, 1, FAR), ("mid", 2, 6, ALL), ("mid", 3, 5, ALL), ("mid", 3, 0, FAR), ("mid", 3, 1, SIDE),
    ("fin", 2, ALL), ("fin", 4, FAR), ("mid", 3, 3, SIDE), ("mid", 3, 3, FAR), ("mid", 3, 6, FAR), ("mid", 3, 6, SIDE),
    ("mid", 3, 4, SIDE), ("mid", 3, 6, OWN), ("mid", 3, 3, OWN), ("fin", 0, ALL), ("mid", 3, 4, OWN), ("fin", 1, ALL),
    ("fin", 5, ALL), ("fin", 3, FAR), ("fin", 3, SIDE), ("fin", 6, FAR), ("fin", 6, SIDE), ("fin", 4, SIDE),
    ("fin", 6, OWN), ("fin", 3, OWN), ("fin", 4, OWN),
)
BF16 = jnp.bfloat16

SPLIT = 3
SPLIT_UNITS = 3
TAILS = (3, 4, 6)
epsilon = 1e-05


def send(src, dst, send_sem, recv_sem, **to):
    return pltpu.make_async_remote_copy(
        src_ref=src, dst_ref=dst, send_sem=send_sem, recv_sem=recv_sem,
        device_id=to, device_id_type=MESH,
    )


def exact_dot(a, b):
    return jnp.dot(a, b, precision=lax.Precision.HIGHEST, preferred_element_type=F32)


def conv_blocks(padded, kernel, out, blocks):
    def columns(i, _):
        cols = pl.ds(pl.multiple_of(i * 256, 256), 256)
        for block in blocks:
            summed = jnp.zeros((64, 256), F32)
            for k in range(4):
                summed = summed + kernel[k : k + 1, cols] * padded[block * 64 + 5 + k : block * 64 + 69 + k, cols]
            out[block * 64 : block * 64 + 64, cols] = (summed * jax.nn.sigmoid(summed)).astype(BF16)
        return 0

    lax.fori_loop(0, out.shape[1] // 256, columns, 0)


def mixer_kernel(
    x_hbm, b_hbm, c_hbm, z_hbm, dt_hbm, conv_x_hbm, conv_b_hbm, conv_c_hbm, rate_hbm, bias_hbm, skip_hbm, gain_hbm, w, out,
    x_in, b_in, c_in, z_in, dt, conv_x, conv_b, conv_c, rate, bias, skip, gain,
    halo_x, halo_b, halo_c, pad_x, pad_b, pad_c, xc, bc, cc, xw,
    step, logd, decay_own, decay, state, state_in, state_out, carried, scores, inside, grow, to_end,
    wg, ag, ring_out, ring_in, done,
    l_sem, h_send, h_recv, d_sem, s_sem, t_sem,
    w_own, w_send, w_recv, wf_send, wf_recv, f_send, f_recv, a_send, a_recv, r_send, r_recv, o_sem,
):
    s, x, y, h = (lax.axis_index(a) for a in ("section", "seq_0", "seq_1", "head"))
    q = x * 4 + y
    ring_at = [[lax.rem(v + o, 4) for o in OFFSETS] for v in (x, y)]
    sides = (lax.rem(h + 1, 8), lax.rem(h + 7, 8))
    peers = [(lax.rem(x + dx, 4), lax.rem(y + dy, 4)) for dx, dy in PEERS]

    barrier = pltpu.get_barrier_semaphore()
    greeted = (
        [{"seq_0": u, "seq_1": v} for u, v in peers]
        + [{"head": v} for v in sides]
        + [{"section": 1 - s, "seq_1": v} for v in ring_at[1]]
        + [{"section": 1 - s, "seq_0": v} for v in ring_at[0][1:]]
    )
    for peer in greeted:
        pl.semaphore_signal(barrier, inc=1, device_id=peer, device_id_type=MESH)

    loads = {}
    for i, (name, src, dst) in enumerate((
        ("dt", dt_hbm, dt), ("bias", bias_hbm, bias), ("rate", rate_hbm, rate),
        ("b", b_hbm, b_in), ("x", x_hbm, x_in), ("c", c_hbm, c_in),
        ("kb", conv_b_hbm, conv_b), ("kx", conv_x_hbm, conv_x), ("kc", conv_c_hbm, conv_c),
        ("skip", skip_hbm, skip), ("z", z_hbm, z_in), ("gain", gain_hbm, gain),
    )):
        loads[name] = pltpu.make_async_copy(src, dst, l_sem.at[i])
        loads[name].start()
    own_w = [pltpu.make_async_copy(w.at[:, pl.ds(a * 256, 256)], wg.at[a, 0], w_own.at[a]) for a in (0, 1)]
    for c in own_w:
        c.start()

    def loaded(*names):
        for n in names:
            loads[n].wait()

    def all_of(ref, sem):
        pltpu.make_async_copy(ref, ref, sem).wait()

    def start(copies):
        for c in copies:
            c.start()

    loaded("b", "x", "c")
    pl.semaphore_wait(barrier, len(greeted))

    to_next = {"seq_0": lax.rem(x + lax.div(y + 1, 4), 4), "seq_1": lax.rem(y + 1, 4)}
    halo = [
        send(src.at[pl.ds(240, 16)], dst, h_send.at[i], h_recv.at[i], **to_next)
        for i, (src, dst) in enumerate(((b_in, halo_b), (x_in, halo_x), (c_in, halo_c)))
    ]

    @pl.when(q < 15)
    def _():
        for c in halo:
            c.start()

    def w_direct(b, low, size, sems):
        rows = pl.ds(low, size)
        copies = []
        for a in (0, 1):
            for slot, to in ((1, 2), (2, 1)):
                copies.append(send(
                    w.at[rows, pl.ds(a * 256 + b * 128, 128)], wg.at[a, slot, rows, pl.ds(b * 128, 128)],
                    sems[0], sems[1], **{SEQ[a]: ring_at[a][to]},
                ))
        return copies

    start(w_direct(0, 0, W_CUT, (w_send, w_recv.at[0])))
    loaded("dt", "bias", "rate")
    row16 = lax.broadcasted_iota(jnp.int32, (16, 16), 0)
    col16 = lax.broadcasted_iota(jnp.int32, (16, 16), 1)

    def column(row):
        return jnp.sum(jnp.where(row16 == col16, jnp.broadcast_to(row, (16, 16)), 0.0), axis=1, keepdims=True)

    raw = dt[...] + column(bias[...])
    step_size = jnp.maximum(raw, 0.0) + jnp.log1p(jnp.exp(-jnp.abs(raw)))
    log_decay = -column(rate[...]) * step_size
    lane = lax.broadcasted_iota(jnp.int32, (16, 256), 1)
    for shift in (1, 2, 4, 8, 16, 32, 64, 128):
        log_decay = log_decay + jnp.where(lane >= shift, pltpu.roll(log_decay, shift, 1), 0.0)
    step[...] = step_size
    logd[...] = log_decay
    spread = jnp.where(
        lax.shift_right_logical(lax.broadcasted_iota(jnp.int32, (16, 1024), 1), 6)
        == lax.broadcasted_iota(jnp.int32, (16, 1024), 0), 1.0, 0.0,
    ).astype(F32)
    log_cols = log_decay.T
    end_cols = (jnp.exp(log_decay[:, 255:256] - log_decay) * step_size).T
    last = exact_dot(jnp.exp(log_cols[248:256, :]), spread)[7:8, :]
    for r in range(8):
        decay_own[r : r + 1, :] = last[:, r * 128 : r * 128 + 128]
    decay[q] = decay_own[...]

    start([
        send(decay_own, decay.at[q], d_sem.at[0], d_sem.at[1], seq_0=u, seq_1=v)
        for i, (u, v) in enumerate(peers)
    ])

    loaded("kb", "kx", "kc", "skip", "z", "gain")
    pad_x[8:264, :] = x_in[...].astype(F32)
    pad_b[8:264, :] = b_in[...].astype(F32)
    pad_c[8:264, :] = c_in[...].astype(F32)
    to_end[...] = exact_dot(end_cols, spread)
    conv_blocks(pad_b, conv_b, bc, (1, 2, 3))
    conv_blocks(pad_x, conv_x, xc, (1, 2, 3))

    def finish(i, halo_ref, padded, kernel, conv_out):
        @pl.when(q > 0)
        def _():
            halo[i].wait_recv()
            padded[0:8, :] = halo_ref[...].astype(F32)[8:16]

        @pl.when(q == 0)
        def _():
            padded[0:8, :] = jnp.zeros((8, padded.shape[1]), F32)

        conv_blocks(padded, kernel, conv_out, (0,))

    finish(0, halo_b, pad_b, conv_b, bc)
    finish(1, halo_x, pad_x, conv_x, xc)

    b_cols = bc[...].astype(F32).T.astype(BF16)
    for i in range(4):
        cols = slice(i * 256, i * 256 + 256)
        xw[:, cols] = (xc[:, cols].astype(F32) * to_end[:, cols]).astype(BF16)
        state[:, cols] = jnp.dot(b_cols, xw[:, cols], preferred_element_type=F32).astype(BF16)
    state_in[q] = state[pl.ds(pl.multiple_of(q * 16, 16), 16), :]
    start([
        send(
            state.at[pl.ds(pl.multiple_of((u * 4 + v) * 16, 16), 16)], state_in.at[q],
            s_sem.at[0], s_sem.at[1], seq_0=u, seq_1=v,
        )
        for i, (u, v) in enumerate(peers)
    ])
    start(w_direct(0, W_CUT, 1024 - W_CUT, (w_send, w_recv.at[0])))

    conv_blocks(pad_c, conv_c, cc, (1, 2, 3))
    finish(2, halo_c, pad_c, conv_c, cc)
    scores[...] = lax.dot_general(cc[...], bc[...], (((1,), (1,)), ((), ())), preferred_element_type=F32)
    skip_row = exact_dot(jnp.broadcast_to(skip[...], (8, 16)), spread)[0:1, :]
    causal = lax.broadcasted_iota(jnp.int32, (128, 128), 0) >= lax.broadcasted_iota(jnp.int32, (128, 128), 1)
    first_half = lax.broadcasted_iota(jnp.int32, (256, 128), 1) < 64
    grow_cols = jnp.exp(log_cols)

    def damped(log_col, head, rows, cols, masked):
        value = jnp.exp(jnp.minimum(log_col[rows] - logd[head : head + 1, cols], 0.0))
        if masked:
            value = jnp.where(causal, value, 0.0)
        return (value * step[head : head + 1, cols] * scores[rows, cols]).astype(BF16)

    top, bottom = slice(0, 128), slice(128, 256)

    def pair(g):
        lanes = slice(g * 128, g * 128 + 128)
        parts = []
        for head in (2 * g, 2 * g + 1):
            log_col = log_cols[:, head : head + 1]
            upper = jnp.dot(damped(log_col, head, top, top, True), xc[top, lanes], preferred_element_type=F32)
            lower = jnp.dot(damped(log_col, head, bottom, top, False), xc[top, lanes], preferred_element_type=F32)
            lower = lower + jnp.dot(damped(log_col, head, bottom, bottom, True), xc[bottom, lanes], preferred_element_type=F32)
            parts.append(jnp.concatenate([upper, lower], axis=0))
        both = jnp.where(first_half, parts[0], parts[1])
        zf = z_in[:, lanes].astype(F32)
        gate = zf * jax.nn.sigmoid(zf)
        inside[:, lanes] = (both + skip_row[:, lanes] * xc[:, lanes].astype(F32)) * gate
        grow[:, lanes] = exact_dot(grow_cols, spread[:, lanes]) * gate

    for g in range(4):
        pair(g)

    all_of(decay.at[pl.ds(0, 15)], d_sem.at[1])
    all_of(state.at[pl.ds(0, 240)], s_sem.at[1])
    for r in range(8):
        lanes = slice(r * 128, r * 128 + 128)
        acc = jnp.zeros((16, 128), F32)
        for k in range(16):
            state_out[k, :, lanes] = acc.astype(BF16)
            if k < 15:
                acc = decay[k, r : r + 1, :] * acc + state_in[k, :, lanes].astype(F32)
    my_rows = pl.ds(pl.multiple_of(q * 16, 16), 16)
    start([
        send(state_out.at[u * 4 + v], carried.at[my_rows], t_sem.at[0], t_sem.at[1], seq_0=u, seq_1=v)
        for i, (u, v) in enumerate(peers)
    ])
    carried[my_rows, :] = state_out[q]

    def w_forward(b):
        cols = pl.ds(b * 128, 128)
        copies = []
        for a in (0, 1):
            for slot, to, low in ((1, 2, 0), (2, 1, 512)):
                at = (pl.ds(low, 512), cols)
                copies.append(send(
                    wg.at[(a, slot, *at)], wg.at[(a, 3, *at)], wf_send, wf_recv.at[b], **{SEQ[a]: ring_at[a][to]},
                ))
        return copies

    for g in range(4, 8):
        pair(g)
    for side in (0, 1):
        for j in range(4):
            for b in (0, 1):
                at = b * 256 + (1 - side) * 128
                ring_in[side, 0, j, :, at : at + 128] = jnp.zeros((128, 128), BF16)
    def a_direct(p):
        copies = []
        for a in (0, 1):
            mine, all_rows = ag.at[a, pl.ds(p * 128, 32)], ag.at[a]
            axis, to = SEQ[1 - a], ring_at[1 - a]
            copies += [
                send(mine, all_rows.at[pl.ds(p * 128 + 32, 32)], a_send.at[0], a_recv.at[0, p], **{axis: to[2]}),
                send(mine, all_rows.at[pl.ds(p * 128 + 64, 32)], a_send.at[0], a_recv.at[0, p], **{axis: to[1]}),
            ]
        return copies

    def a_forward(p):
        copies = []
        for a in (0, 1):
            rows = ag.at[a]
            axis, to = SEQ[1 - a], ring_at[1 - a]
            copies += [
                send(rows.at[pl.ds(p * 128 + 32, 16)], rows.at[pl.ds(p * 128 + 96, 16)], a_send.at[1], a_recv.at[1, p], **{axis: to[2]}),
                send(rows.at[pl.ds(p * 128 + 80, 16)], rows.at[pl.ds(p * 128 + 112, 16)], a_send.at[1], a_recv.at[1, p], **{axis: to[1]}),
            ]
        return copies

    direct = {p: a_direct(p) for p in range(8)}
    passed = {p: a_forward(p) for p in range(8)}

    all_of(state.at[pl.ds(0, 240)], t_sem.at[1])

    def hidden(p):
        rows = pl.ds(pl.multiple_of(lax.rem(h + PIECES[p], 8) * 32, 32), 32)
        outside = jnp.dot(cc[rows, :], carried[...], preferred_element_type=F32)
        gated = inside[rows, :] + outside * grow[rows, :]
        inverse_rms = lax.rsqrt(jnp.mean(gated * gated, axis=1, keepdims=True) + epsilon)
        value = (gated * inverse_rms * gain[...]).astype(BF16)
        ag[0, p * 128 : p * 128 + 32, :] = value
        ag[1, p * 128 : p * 128 + 32, :] = value

    seen, ring_seen = set(), set()

    def need(key):
        if key in seen:
            return
        seen.add(key)
        kind, index = key
        if kind == "own":
            for c in own_w:
                c.wait()
        if kind == "direct":
            all_of(ag.at[0, pl.ds(0, 128)], a_recv.at[0, index])
        if kind == "passed":
            all_of(ag.at[0, pl.ds(0, 64)], a_recv.at[1, index])
        if kind == "w":
            all_of(ag.at[0, pl.ds(0, 512)], w_recv.at[index])
        if kind == "wf":
            all_of(ag.at[0, pl.ds(0, 256)], wf_recv.at[index])

    def need_rows(p, group):
        if group != OWN:
            need(("direct", p))
        if group in (ALL, FAR):
            need(("passed", p))

    def need_w(u):
        j, b = UNITS[u]
        need(("own", 0))
        if j in (1, 2):
            need(("w", b))
        if j == 3:
            need(("wf", b))

    def unit_cols(u):
        b = UNITS[u][1]
        return (0, 512) if b is None else (b * 256, 256)

    def halves(u):
        b = UNITS[u][1]
        return (0, 1) if b is None else (b,)

    def products(low, size, u):
        j, b = UNITS[u]
        cols = slice(0, 256) if b is None else slice(b * 128, b * 128 + 128)
        parts = []
        for a in (0, 1):
            part = jnp.dot(ag[a, low : low + size, :], wg[a, j, :, cols], preferred_element_type=F32)
            parts.append({v: part[:, i * 128 : i * 128 + 128] for i, v in enumerate(halves(u))})
        return parts

    def first(u, group):
        low, size = group
        j = UNITS[u][0]
        need_w(u)
        if group != OWN:
            need_rows(0, group)
        parts = products(low, size, u)
        copies = []
        for a in (0, 1):
            for b in halves(u):
                at = b * 256 + a * 128
                ring_out[a, 0, j, low : low + size, at : at + 128] = parts[a][b].astype(BF16)
                rows, cols = pl.ds(low, size), pl.ds(at, 128)
                copies.append(send(
                    ring_out.at[a, 0, j, rows, cols], ring_in.at[a, 0, j, rows, cols],
                    f_send, f_recv.at[u, SLOT[group]], **{"head": sides[a]},
                ))
        start(copies)

    def ring_need(stage, u, group):
        groups = (OWN, SIDE, FAR) if split(stage, u) else (ALL,)
        for waited in groups:
            if group in (ALL, waited) or waited == ALL:
                if (stage, u, waited) not in ring_seen:
                    ring_seen.add((stage, u, waited))
                    ring_wait(stage, u, waited)

    def ring_wait(stage, u, group):
        low, size = group
        n = unit_cols(u)[1]
        sem = (f_recv.at[u, SLOT[group]] if stage == 0 else r_recv.at[stage - 1, u, SLOT[group]])
        if stage == 0:
            all_of(ring_in.at[0, 0, 0, pl.ds(low, size), pl.ds(0, n)], sem)
        else:
            all_of(ring_in.at[0, 0, pl.ds(0, 2), pl.ds(low, size), pl.ds(0, n)], sem)

    def middle(stage, u, group=ALL):
        p = 2 * stage - 1
        low, size = group
        j = UNITS[u][0]
        need_w(u)
        need_rows(p, group)
        need_rows(p + 1, group)
        if group == ALL:
            both = products(p * 128, 256, u)
            parts = [[{b: both[a][b][side * 128 : side * 128 + 128] for b in halves(u)} for a in (0, 1)] for side in (0, 1)]
        else:
            parts = [products((p + side) * 128 + low, size, u) for side in (0, 1)]
        ring_need(stage - 1, u, group)
        rows = slice(low, low + size)
        for side in (0, 1):
            for b in halves(u):
                for a in (0, 1):
                    cols = slice(b * 256 + a * 128, b * 256 + a * 128 + 128)
                    got = ring_in[side, stage - 1, j, rows, cols].astype(F32)
                    ring_out[side, stage, j, rows, cols] = (parts[side][a][b] + got).astype(BF16)
        at = (pl.ds(low, size), pl.ds(*unit_cols(u)))
        start([
            send(
                ring_out.at[(side, stage, j, *at)], ring_in.at[(side, stage, j, *at)],
                r_send, r_recv.at[stage - 1, u, SLOT[group]], **{"head": sides[side]},
            )
            for side in (0, 1)
        ])

    def split(stage, u):
        return (u < SPLIT_UNITS and stage <= SPLIT) or (u in TAILS and stage == 3)

    def final(u, group):
        j, b = UNITS[u]
        first_row, size = group
        rows = slice(first_row, first_row + size)
        need_w(u)
        need_rows(7, group)
        parts = products(896 + first_row, size, u)
        ring_need(3, u, group)
        low, n = (0, 256) if b is None else (b * 128, 128)
        copies = []
        for a in (0, 1):
            for v in halves(u):
                at = v * 256 + a * 128
                total = parts[a][v]
                for side in (0, 1):
                    total = total + ring_in[side, 3, j, rows, at : at + 128].astype(F32)
                done[a, j, rows, v * 128 : v * 128 + 128] = total.astype(BF16)
            shard = ring_at[0][j] * 4 + y if a == 0 else x * 4 + ring_at[1][j]
            cols = pl.ds(pl.multiple_of(shard * 512 + a * 256 + low, 128), n)
            for r in (3, 1, 2, 0):
                if first_row <= r * 32 < first_row + size:
                    axis = {SEQ[1 - a]: ring_at[1 - a][r]}
                    copies.append(send(
                        done.at[a, j, pl.ds(r * 32, 32), pl.ds(low, n)], out.at[:, cols], o_sem.at[0], o_sem.at[1], section=1 - s, **axis
                    ))
        start(copies)

    for op, *at in ORDER:
        if op == "hd":
            hidden(*at)
            start(direct[at[0]])
        if op == "fw":
            need(("direct", *at))
            start(passed[at[0]])
        if op == "wf":
            need(("w", *at))
            start(w_forward(*at))
        if op == "wb":
            start(w_direct(1, at[0] * 256, 256, (w_send, w_recv.at[1])))
        if op == "first":
            first(*at)
        if op == "mid":
            middle(*at)
        if op == "fin":
            final(*at)

    all_of(decay.at[pl.ds(0, 15)], d_sem.at[0])
    all_of(state.at[pl.ds(0, 240)], s_sem.at[0])
    all_of(state.at[pl.ds(0, 240)], t_sem.at[0])
    all_of(ag.at[0], w_send)
    all_of(ag.at[0, pl.ds(0, 512)], wf_send)
    all_of(ag.at[0, pl.ds(0, 256)], f_send)
    all_of(ag.at[0], a_send.at[0])
    all_of(ag.at[0, pl.ds(0, 512)], a_send.at[1])
    all_of(ring_out.at[:, pl.ds(1, 3)], r_send)
    all_of(done, o_sem.at[0])

    @pl.when(q < 15)
    def _():
        for c in halo:
            c.wait_send()

    all_of(out, o_sem.at[1])


def per_device(
    x_in, b_in, c_in, z_in, dt_raw, conv_x, conv_b, conv_c, a_rate, dt_bias, skip_d, norm_gain, out_weight
):
    dma = pltpu.SemaphoreType.DMA
    half = lambda *shape: pltpu.VMEM(shape, BF16)
    full = lambda *shape: pltpu.VMEM(shape, F32)
    anywhere = pl.BlockSpec(memory_space=pl.ANY)
    mixed = pl.pallas_call(
        mixer_kernel,
        out_shape=pltpu.VMEM((32, 8192), BF16),
        in_specs=[anywhere] * 13,
        out_specs=pl.BlockSpec(memory_space=pltpu.VMEM),
        scratch_shapes=[
            half(256, 1024), half(256, 256), half(256, 256), half(256, 1024), full(16, 256),
            full(4, 1024), full(4, 256), full(4, 256), full(1, 16), full(1, 16), full(1, 16), full(1, 1024),
            half(16, 1024), half(16, 256), half(16, 256), full(264, 1024), full(264, 256), full(264, 256),
            half(256, 1024), half(256, 256), half(256, 256), half(256, 1024),
            full(16, 256), full(16, 256), full(8, 128), full(16, 8, 128),
            half(256, 1024), half(16, 16, 1024), half(16, 16, 1024), half(256, 1024),
            full(256, 256), full(256, 1024), full(256, 1024), full(256, 1024),
            half(2, 4, 1024, 256), half(2, 1024, 1024), half(2, 4, 4, 128, 512), half(2, 4, 4, 128, 512), half(2, 4, 128, 256),
            dma((12,)), dma((3,)), dma((3,)), dma((2,)), dma((2,)), dma((2,)),
            dma((2,)), dma, dma((2,)), dma, dma((2,)), dma, dma((7, 3)), dma((2,)), dma((2, 8)), dma, dma((3, 7, 3)), dma((2,)),
        ],
        compiler_params=pltpu.CompilerParams(
            collective_id=0, has_side_effects=True, vmem_limit_bytes=56 * 2**20
        ),
    )(
        x_in[0], b_in[0], c_in[0], z_in[0], dt_raw[0], conv_x[0], conv_b[0], conv_c[0],
        a_rate, dt_bias, skip_d, norm_gain, out_weight[0],
    )
    return mixed[None]


def solution(mesh):
    finer = Mesh(
        mesh.devices.reshape(mesh.shape["section"], 4, 4, mesh.shape["head"]),
        ("section", "seq_0", "seq_1", "head"),
    )
    return jax.shard_map(
        per_device,
        mesh=finer,
        in_specs=(
            P("section", SEQ, "head"),
            P("section", SEQ, "head"),
            P("section", SEQ, "head"),
            P("section", SEQ, "head"),
            P("section", "head", SEQ),
            P("section", None, "head"),
            P("section", None, "head"),
            P("section", None, "head"),
            P("section", "head"),
            P("section", "head"),
            P("section", "head"),
            P("section", "head"),
            P("section", "head", SEQ),
        ),
        out_specs=P("section", SEQ_HEAD, None),
        check_vma=False,
    )
```

```python
import jax
import jax.numpy as jnp
from jax import lax
from jax.experimental import pallas as pl
from jax.experimental.pallas import tpu as pltpu
from jax.sharding import Mesh
from jax.sharding import PartitionSpec as P

SEQ = ("seq_0", "seq_1")
SEQ_HEAD = ("seq_0", "seq_1", "head")
MESH = pl.DeviceIdType.MESH
PIECES = (4, 3, 5, 2, 6, 1, 7, 0)
OFFSETS = (0, 3, 1, 2)
PEERS = (
    (2, 2), (1, 2), (3, 2), (2, 1), (2, 3), (0, 2), (2, 0), (1, 1), (3, 3), (1, 3), (3, 1), (0, 1), (3, 0), (0, 3), (1, 0),
)
W_CUT = 672
UNITS = ((0, None), (1, 0), (2, 0), (1, 1), (2, 1), (3, 0), (3, 1))
ALL, FAR, OWN, SIDE = (0, 128), (96, 32), (0, 32), (32, 64)
SLOT = {ALL: 0, OWN: 0, SIDE: 1, FAR: 2}
F32 = jnp.float32
ORDER = (
    ("wb", 2), ("hd", 0), ("first", 2, OWN), ("hd", 1), ("first", 0, OWN), ("hd", 2),
    ("first", 1, OWN), ("wb", 0), ("mid", 1, 2, OWN), ("mid", 1, 0, OWN), ("mid", 1, 1, OWN), ("first", 0, SIDE),
    ("first", 1, SIDE), ("fw", 0), ("wb", 3), ("wb", 1), ("hd", 4), ("hd", 3),
    ("first", 2, SIDE), ("mid", 2, 2, OWN), ("mid", 2, 0, OWN), ("mid", 2, 1, OWN), ("fw", 1), ("fw", 2),
    ("mid", 1, 0, SIDE), ("wf", 0), ("mid", 1, 1, SIDE), ("hd", 6), ("hd", 5), ("first", 2, FAR),
    ("first", 1, FAR), ("mid", 3, 2, OWN), ("mid", 1, 2, SIDE), ("mid", 3, 0, OWN), ("first", 4, ALL), ("first", 3, ALL),
    ("mid", 3, 1, OWN), ("wf", 1), ("first", 0, FAR), ("mid", 2, 0, SIDE), ("fw", 4), ("mid", 2, 1, SIDE),
    ("fw", 3), ("mid", 2, 2, SIDE), ("mid", 1, 4, ALL), ("mid", 1, 1, FAR), ("first", 5, ALL), ("mid", 1, 0, FAR),
    ("mid", 1, 3, ALL), ("mid", 3, 2, SIDE), ("mid", 3, 0, SIDE), ("hd", 7), ("fw", 5), ("mid", 1, 2, FAR),
    ("first", 6, ALL), ("fw", 6), ("mid", 1, 5, ALL), ("mid", 2, 4, ALL), ("mid", 2, 1, FAR), ("mid", 2, 0, FAR),
    ("mid", 2, 2, FAR), ("mid", 1, 6, ALL), ("mid", 2, 5, ALL), ("mid", 2, 3, ALL), ("mid", 3, 4, FAR), ("fw", 7),
    ("mid", 3, 2, FAR), ("mid", 3, 1, FAR), ("mid", 2, 6, ALL), ("mid", 3, 5, ALL), ("mid", 3, 0, FAR), ("mid", 3, 1, SIDE),
    ("fin", 2, ALL), ("fin", 4, FAR), ("mid", 3, 3, SIDE), ("mid", 3, 3, FAR), ("mid", 3, 6, FAR), ("mid", 3, 6, SIDE),
    ("mid", 3, 4, SIDE), ("mid", 3, 6, OWN), ("mid", 3, 3, OWN), ("fin", 0, ALL), ("mid", 3, 4, OWN), ("fin", 1, ALL),
    ("fin", 5, ALL), ("fin", 3, FAR), ("fin", 3, SIDE), ("fin", 6, FAR), ("fin", 6, SIDE), ("fin", 4, SIDE),
    ("fin", 6, OWN), ("fin", 3, OWN), ("fin", 4, OWN),
)
BF16 = jnp.bfloat16

SPLIT = 3
SPLIT_UNITS = 3
TAILS = (3, 4, 6)
epsilon = 1e-05


def send(src, dst, send_sem, recv_sem, **to):
    return pltpu.make_async_remote_copy(
        src_ref=src, dst_ref=dst, send_sem=send_sem, recv_sem=recv_sem,
        device_id=to, device_id_type=MESH,
    )


def exact_dot(a, b):
    return jnp.dot(a, b, precision=lax.Precision.HIGHEST, preferred_element_type=F32)


def conv_blocks(padded, kernel, out, blocks):
    def columns(i, _):
        cols = pl.ds(pl.multiple_of(i * 256, 256), 256)
        for block in blocks:
            summed = jnp.zeros((64, 256), F32)
            for k in range(4):
                summed = summed + kernel[k : k + 1, cols] * padded[block * 64 + 5 + k : block * 64 + 69 + k, cols]
            out[block * 64 : block * 64 + 64, cols] = (summed * jax.nn.sigmoid(summed)).astype(BF16)
        return 0

    lax.fori_loop(0, out.shape[1] // 256, columns, 0)


def mixer_kernel(
    x_hbm, b_hbm, c_hbm, z_hbm, dt_hbm, conv_x_hbm, conv_b_hbm, conv_c_hbm, rate_hbm, bias_hbm, skip_hbm, gain_hbm, w, out,
    x_in, b_in, c_in, z_in, dt, conv_x, conv_b, conv_c, rate, bias, skip, gain,
    halo_x, halo_b, halo_c, pad_x, pad_b, pad_c, xc, bc, cc, xw,
    step, logd, decay_own, decay, state, state_in, state_out, carried, scores, inside, grow, to_end,
    wg, ag, ring_out, ring_in, done,
    l_sem, h_send, h_recv, d_sem, s_sem, t_sem,
    w_own, w_send, w_recv, wf_send, wf_recv, f_send, f_recv, a_send, a_recv, r_send, r_recv, o_sem,
):
    s, x, y, h = (lax.axis_index(a) for a in ("section", "seq_0", "seq_1", "head"))
    q = x * 4 + y
    ring_at = [[lax.rem(v + o, 4) for o in OFFSETS] for v in (x, y)]
    sides = (lax.rem(h + 1, 8), lax.rem(h + 7, 8))
    peers = [(lax.rem(x + dx, 4), lax.rem(y + dy, 4)) for dx, dy in PEERS]

    barrier = pltpu.get_barrier_semaphore()
    greeted = (
        [{"seq_0": u, "seq_1": v} for u, v in peers]
        + [{"head": v} for v in sides]
        + [{"section": 1 - s, "seq_1": v} for v in ring_at[1]]
        + [{"section": 1 - s, "seq_0": v} for v in ring_at[0][1:]]
    )
    for peer in greeted:
        pl.semaphore_signal(barrier, inc=1, device_id=peer, device_id_type=MESH)

    loads = {}
    for i, (name, src, dst) in enumerate((
        ("dt", dt_hbm, dt), ("bias", bias_hbm, bias), ("rate", rate_hbm, rate),
        ("b", b_hbm, b_in), ("x", x_hbm, x_in), ("c", c_hbm, c_in),
        ("kb", conv_b_hbm, conv_b), ("kx", conv_x_hbm, conv_x), ("kc", conv_c_hbm, conv_c),
        ("skip", skip_hbm, skip), ("z", z_hbm, z_in), ("gain", gain_hbm, gain),
    )):
        loads[name] = pltpu.make_async_copy(src, dst, l_sem.at[i])
        loads[name].start()
    own_w = [pltpu.make_async_copy(w.at[:, pl.ds(a * 256, 256)], wg.at[a, 0], w_own.at[a]) for a in (0, 1)]
    for c in own_w:
        c.start()

    def loaded(*names):
        for n in names:
            loads[n].wait()

    def all_of(ref, sem):
        pltpu.make_async_copy(ref, ref, sem).wait()

    def start(copies):
        for c in copies:
            c.start()

    loaded("b", "x", "c")
    pl.semaphore_wait(barrier, len(greeted))

    to_next = {"seq_0": lax.rem(x + lax.div(y + 1, 4), 4), "seq_1": lax.rem(y + 1, 4)}
    halo = [
        send(src.at[pl.ds(248, 8)], dst, h_send.at[i], h_recv.at[i], **to_next)
        for i, (src, dst) in enumerate(((b_in, halo_b), (x_in, halo_x), (c_in, halo_c)))
    ]

    @pl.when(q < 15)
    def _():
        for c in halo:
            c.start()

    def w_direct(b, low, size, sems):
        rows = pl.ds(low, size)
        copies = []
        for a in (0, 1):
            for slot, to in ((1, 2), (2, 1)):
                copies.append(send(
                    w.at[rows, pl.ds(a * 256 + b * 128, 128)], wg.at[a, slot, rows, pl.ds(b * 128, 128)],
                    sems[0], sems[1], **{SEQ[a]: ring_at[a][to]},
                ))
        return copies

    start(w_direct(0, 0, W_CUT, (w_send, w_recv.at[0])))
    loaded("dt", "bias", "rate")
    row16 = lax.broadcasted_iota(jnp.int32, (16, 16), 0)
    col16 = lax.broadcasted_iota(jnp.int32, (16, 16), 1)

    def column(row):
        return jnp.sum(jnp.where(row16 == col16, jnp.broadcast_to(row, (16, 16)), 0.0), axis=1, keepdims=True)

    raw = dt[...] + column(bias[...])
    step_size = jnp.maximum(raw, 0.0) + jnp.log1p(jnp.exp(-jnp.abs(raw)))
    log_decay = -column(rate[...]) * step_size
    lane = lax.broadcasted_iota(jnp.int32, (16, 256), 1)
    for shift in (1, 2, 4, 8, 16, 32, 64, 128):
        log_decay = log_decay + jnp.where(lane >= shift, pltpu.roll(log_decay, shift, 1), 0.0)
    step[...] = step_size
    logd[...] = log_decay
    spread = jnp.where(
        lax.shift_right_logical(lax.broadcasted_iota(jnp.int32, (16, 1024), 1), 6)
        == lax.broadcasted_iota(jnp.int32, (16, 1024), 0), 1.0, 0.0,
    ).astype(F32)
    log_cols = log_decay.T
    end_cols = (jnp.exp(log_decay[:, 255:256] - log_decay) * step_size).T
    last = exact_dot(jnp.exp(log_cols[248:256, :]), spread)[7:8, :]
    for r in range(8):
        decay_own[r : r + 1, :] = last[:, r * 128 : r * 128 + 128]
    decay[q] = decay_own[...]

    start([
        send(decay_own, decay.at[q], d_sem.at[0], d_sem.at[1], seq_0=u, seq_1=v)
        for i, (u, v) in enumerate(peers)
    ])

    loaded("kb", "kx", "kc", "skip", "z", "gain")
    pad_x[8:264, :] = x_in[...].astype(F32)
    pad_b[8:264, :] = b_in[...].astype(F32)
    pad_c[8:264, :] = c_in[...].astype(F32)
    to_end[...] = exact_dot(end_cols, spread)
    conv_blocks(pad_b, conv_b, bc, (1, 2, 3))
    conv_blocks(pad_x, conv_x, xc, (1, 2, 3))

    def finish(i, halo_ref, padded, kernel, conv_out):
        @pl.when(q > 0)
        def _():
            halo[i].wait_recv()
            padded[0:8, :] = halo_ref[...].astype(F32)

        @pl.when(q == 0)
        def _():
            padded[0:8, :] = jnp.zeros((8, padded.shape[1]), F32)

        conv_blocks(padded, kernel, conv_out, (0,))

    finish(0, halo_b, pad_b, conv_b, bc)
    finish(1, halo_x, pad_x, conv_x, xc)

    b_cols = bc[...].astype(F32).T.astype(BF16)
    for i in range(4):
        cols = slice(i * 256, i * 256 + 256)
        xw[:, cols] = (xc[:, cols].astype(F32) * to_end[:, cols]).astype(BF16)
        state[:, cols] = jnp.dot(b_cols, xw[:, cols], preferred_element_type=F32).astype(BF16)
    state_in[q] = state[pl.ds(pl.multiple_of(q * 16, 16), 16), :]
    start([
        send(
            state.at[pl.ds(pl.multiple_of((u * 4 + v) * 16, 16), 16)], state_in.at[q],
            s_sem.at[0], s_sem.at[1], seq_0=u, seq_1=v,
        )
        for i, (u, v) in enumerate(peers)
    ])
    start(w_direct(0, W_CUT, 1024 - W_CUT, (w_send, w_recv.at[0])))

    conv_blocks(pad_c, conv_c, cc, (1, 2, 3))
    finish(2, halo_c, pad_c, conv_c, cc)
    scores[...] = lax.dot_general(cc[...], bc[...], (((1,), (1,)), ((), ())), preferred_element_type=F32)
    skip_row = exact_dot(jnp.broadcast_to(skip[...], (8, 16)), spread)[0:1, :]
    causal = lax.broadcasted_iota(jnp.int32, (128, 128), 0) >= lax.broadcasted_iota(jnp.int32, (128, 128), 1)
    first_half = lax.broadcasted_iota(jnp.int32, (256, 128), 1) < 64
    grow_cols = jnp.exp(log_cols)

    def damped(log_col, head, rows, cols, masked):
        value = jnp.exp(jnp.minimum(log_col[rows] - logd[head : head + 1, cols], 0.0))
        if masked:
            value = jnp.where(causal, value, 0.0)
        return (value * step[head : head + 1, cols] * scores[rows, cols]).astype(BF16)

    top, bottom = slice(0, 128), slice(128, 256)

    def pair(g):
        lanes = slice(g * 128, g * 128 + 128)
        parts = []
        for head in (2 * g, 2 * g + 1):
            log_col = log_cols[:, head : head + 1]
            upper = jnp.dot(damped(log_col, head, top, top, True), xc[top, lanes], preferred_element_type=F32)
            lower = jnp.dot(damped(log_col, head, bottom, top, False), xc[top, lanes], preferred_element_type=F32)
            lower = lower + jnp.dot(damped(log_col, head, bottom, bottom, True), xc[bottom, lanes], preferred_element_type=F32)
            parts.append(jnp.concatenate([upper, lower], axis=0))
        both = jnp.where(first_half, parts[0], parts[1])
        zf = z_in[:, lanes].astype(F32)
        gate = zf * jax.nn.sigmoid(zf)
        inside[:, lanes] = (both + skip_row[:, lanes] * xc[:, lanes].astype(F32)) * gate
        grow[:, lanes] = exact_dot(grow_cols, spread[:, lanes]) * gate

    for g in range(4):
        pair(g)

    all_of(decay.at[pl.ds(0, 15)], d_sem.at[1])
    all_of(state.at[pl.ds(0, 240)], s_sem.at[1])
    for r in range(8):
        lanes = slice(r * 128, r * 128 + 128)
        acc = jnp.zeros((16, 128), F32)
        for k in range(16):
            state_out[k, :, lanes] = acc.astype(BF16)
            if k < 15:
                acc = decay[k, r : r + 1, :] * acc + state_in[k, :, lanes].astype(F32)
    my_rows = pl.ds(pl.multiple_of(q * 16, 16), 16)
    start([
        send(state_out.at[u * 4 + v], carried.at[my_rows], t_sem.at[0], t_sem.at[1], seq_0=u, seq_1=v)
        for i, (u, v) in enumerate(peers)
    ])
    carried[my_rows, :] = state_out[q]

    def w_forward(b):
        cols = pl.ds(b * 128, 128)
        copies = []
        for a in (0, 1):
            for slot, to, low in ((1, 2, 0), (2, 1, 512)):
                at = (pl.ds(low, 512), cols)
                copies.append(send(
                    wg.at[(a, slot, *at)], wg.at[(a, 3, *at)], wf_send, wf_recv.at[b], **{SEQ[a]: ring_at[a][to]},
                ))
        return copies

    for g in range(4, 8):
        pair(g)
    for side in (0, 1):
        for j in range(4):
            for b in (0, 1):
                at = b * 256 + (1 - side) * 128
                ring_in[side, 0, j, :, at : at + 128] = jnp.zeros((128, 128), BF16)
    def a_direct(p):
        copies = []
        for a in (0, 1):
            mine, all_rows = ag.at[a, pl.ds(p * 128, 32)], ag.at[a]
            axis, to = SEQ[1 - a], ring_at[1 - a]
            copies += [
                send(mine, all_rows.at[pl.ds(p * 128 + 32, 32)], a_send.at[0], a_recv.at[0, p], **{axis: to[2]}),
                send(mine, all_rows.at[pl.ds(p * 128 + 64, 32)], a_send.at[0], a_recv.at[0, p], **{axis: to[1]}),
            ]
        return copies

    def a_forward(p):
        copies = []
        for a in (0, 1):
            rows = ag.at[a]
            axis, to = SEQ[1 - a], ring_at[1 - a]
            copies += [
                send(rows.at[pl.ds(p * 128 + 32, 16)], rows.at[pl.ds(p * 128 + 96, 16)], a_send.at[1], a_recv.at[1, p], **{axis: to[2]}),
                send(rows.at[pl.ds(p * 128 + 80, 16)], rows.at[pl.ds(p * 128 + 112, 16)], a_send.at[1], a_recv.at[1, p], **{axis: to[1]}),
            ]
        return copies

    direct = {p: a_direct(p) for p in range(8)}
    passed = {p: a_forward(p) for p in range(8)}

    all_of(state.at[pl.ds(0, 240)], t_sem.at[1])

    def hidden(p):
        rows = pl.ds(pl.multiple_of(lax.rem(h + PIECES[p], 8) * 32, 32), 32)
        outside = jnp.dot(cc[rows, :], carried[...], preferred_element_type=F32)
        gated = inside[rows, :] + outside * grow[rows, :]
        inverse_rms = lax.rsqrt(jnp.mean(gated * gated, axis=1, keepdims=True) + epsilon)
        value = (gated * inverse_rms * gain[...]).astype(BF16)
        ag[0, p * 128 : p * 128 + 32, :] = value
        ag[1, p * 128 : p * 128 + 32, :] = value

    seen, ring_seen = set(), set()

    def need(key):
        if key in seen:
            return
        seen.add(key)
        kind, index = key
        if kind == "own":
            for c in own_w:
                c.wait()
        if kind == "direct":
            all_of(ag.at[0, pl.ds(0, 128)], a_recv.at[0, index])
        if kind == "passed":
            all_of(ag.at[0, pl.ds(0, 64)], a_recv.at[1, index])
        if kind == "w":
            all_of(ag.at[0, pl.ds(0, 512)], w_recv.at[index])
        if kind == "wf":
            all_of(ag.at[0, pl.ds(0, 256)], wf_recv.at[index])

    def need_rows(p, group):
        if group != OWN:
            need(("direct", p))
        if group in (ALL, FAR):
            need(("passed", p))

    def need_w(u):
        j, b = UNITS[u]
        need(("own", 0))
        if j in (1, 2):
            need(("w", b))
        if j == 3:
            need(("wf", b))

    def unit_cols(u):
        b = UNITS[u][1]
        return (0, 512) if b is None else (b * 256, 256)

    def halves(u):
        b = UNITS[u][1]
        return (0, 1) if b is None else (b,)

    def products(low, size, u):
        j, b = UNITS[u]
        cols = slice(0, 256) if b is None else slice(b * 128, b * 128 + 128)
        parts = []
        for a in (0, 1):
            part = jnp.dot(ag[a, low : low + size, :], wg[a, j, :, cols], preferred_element_type=F32)
            parts.append({v: part[:, i * 128 : i * 128 + 128] for i, v in enumerate(halves(u))})
        return parts

    def first(u, group):
        low, size = group
        j = UNITS[u][0]
        need_w(u)
        if group != OWN:
            need_rows(0, group)
        parts = products(low, size, u)
        copies = []
        for a in (0, 1):
            for b in halves(u):
                at = b * 256 + a * 128
                ring_out[a, 0, j, low : low + size, at : at + 128] = parts[a][b].astype(BF16)
                rows, cols = pl.ds(low, size), pl.ds(at, 128)
                copies.append(send(
                    ring_out.at[a, 0, j, rows, cols], ring_in.at[a, 0, j, rows, cols],
                    f_send, f_recv.at[u, SLOT[group]], **{"head": sides[a]},
                ))
        start(copies)

    def ring_need(stage, u, group):
        groups = (OWN, SIDE, FAR) if split(stage, u) else (ALL,)
        for waited in groups:
            if group in (ALL, waited) or waited == ALL:
                if (stage, u, waited) not in ring_seen:
                    ring_seen.add((stage, u, waited))
                    ring_wait(stage, u, waited)

    def ring_wait(stage, u, group):
        low, size = group
        n = unit_cols(u)[1]
        sem = (f_recv.at[u, SLOT[group]] if stage == 0 else r_recv.at[stage - 1, u, SLOT[group]])
        if stage == 0:
            all_of(ring_in.at[0, 0, 0, pl.ds(low, size), pl.ds(0, n)], sem)
        else:
            all_of(ring_in.at[0, 0, pl.ds(0, 2), pl.ds(low, size), pl.ds(0, n)], sem)

    def middle(stage, u, group=ALL):
        p = 2 * stage - 1
        low, size = group
        j = UNITS[u][0]
        need_w(u)
        need_rows(p, group)
        need_rows(p + 1, group)
        if group == ALL:
            both = products(p * 128, 256, u)
            parts = [[{b: both[a][b][side * 128 : side * 128 + 128] for b in halves(u)} for a in (0, 1)] for side in (0, 1)]
        else:
            parts = [products((p + side) * 128 + low, size, u) for side in (0, 1)]
        ring_need(stage - 1, u, group)
        rows = slice(low, low + size)
        for side in (0, 1):
            for b in halves(u):
                for a in (0, 1):
                    cols = slice(b * 256 + a * 128, b * 256 + a * 128 + 128)
                    got = ring_in[side, stage - 1, j, rows, cols].astype(F32)
                    ring_out[side, stage, j, rows, cols] = (parts[side][a][b] + got).astype(BF16)
        at = (pl.ds(low, size), pl.ds(*unit_cols(u)))
        start([
            send(
                ring_out.at[(side, stage, j, *at)], ring_in.at[(side, stage, j, *at)],
                r_send, r_recv.at[stage - 1, u, SLOT[group]], **{"head": sides[side]},
            )
            for side in (0, 1)
        ])

    def split(stage, u):
        return (u < SPLIT_UNITS and stage <= SPLIT) or (u in TAILS and stage == 3)

    def final(u, group):
        j, b = UNITS[u]
        first_row, size = group
        rows = slice(first_row, first_row + size)
        need_w(u)
        need_rows(7, group)
        parts = products(896 + first_row, size, u)
        ring_need(3, u, group)
        low, n = (0, 256) if b is None else (b * 128, 128)
        copies = []
        for a in (0, 1):
            for v in halves(u):
                at = v * 256 + a * 128
                total = parts[a][v]
                for side in (0, 1):
                    total = total + ring_in[side, 3, j, rows, at : at + 128].astype(F32)
                done[a, j, rows, v * 128 : v * 128 + 128] = total.astype(BF16)
            shard = ring_at[0][j] * 4 + y if a == 0 else x * 4 + ring_at[1][j]
            cols = pl.ds(pl.multiple_of(shard * 512 + a * 256 + low, 128), n)
            for r in (3, 1, 2, 0):
                if first_row <= r * 32 < first_row + size:
                    axis = {SEQ[1 - a]: ring_at[1 - a][r]}
                    copies.append(send(
                        done.at[a, j, pl.ds(r * 32, 32), pl.ds(low, n)], out.at[:, cols], o_sem.at[0], o_sem.at[1], section=1 - s, **axis
                    ))
        start(copies)

    for op, *at in ORDER:
        if op == "hd":
            hidden(*at)
            start(direct[at[0]])
        if op == "fw":
            need(("direct", *at))
            start(passed[at[0]])
        if op == "wf":
            need(("w", *at))
            start(w_forward(*at))
        if op == "wb":
            start(w_direct(1, at[0] * 256, 256, (w_send, w_recv.at[1])))
        if op == "first":
            first(*at)
        if op == "mid":
            middle(*at)
        if op == "fin":
            final(*at)

    all_of(decay.at[pl.ds(0, 15)], d_sem.at[0])
    all_of(state.at[pl.ds(0, 240)], s_sem.at[0])
    all_of(state.at[pl.ds(0, 240)], t_sem.at[0])
    all_of(ag.at[0], w_send)
    all_of(ag.at[0, pl.ds(0, 512)], wf_send)
    all_of(ag.at[0, pl.ds(0, 256)], f_send)
    all_of(ag.at[0], a_send.at[0])
    all_of(ag.at[0, pl.ds(0, 512)], a_send.at[1])
    all_of(ring_out.at[:, pl.ds(1, 3)], r_send)
    all_of(done, o_sem.at[0])

    @pl.when(q < 15)
    def _():
        for c in halo:
            c.wait_send()

    all_of(out, o_sem.at[1])


def per_device(
    x_in, b_in, c_in, z_in, dt_raw, conv_x, conv_b, conv_c, a_rate, dt_bias, skip_d, norm_gain, out_weight
):
    dma = pltpu.SemaphoreType.DMA
    half = lambda *shape: pltpu.VMEM(shape, BF16)
    full = lambda *shape: pltpu.VMEM(shape, F32)
    anywhere = pl.BlockSpec(memory_space=pl.ANY)
    mixed = pl.pallas_call(
        mixer_kernel,
        out_shape=pltpu.VMEM((32, 8192), BF16),
        in_specs=[anywhere] * 13,
        out_specs=pl.BlockSpec(memory_space=pltpu.VMEM),
        scratch_shapes=[
            half(256, 1024), half(256, 256), half(256, 256), half(256, 1024), full(16, 256),
            full(4, 1024), full(4, 256), full(4, 256), full(1, 16), full(1, 16), full(1, 16), full(1, 1024),
            half(8, 1024), half(8, 256), half(8, 256), full(264, 1024), full(264, 256), full(264, 256),
            half(256, 1024), half(256, 256), half(256, 256), half(256, 1024),
            full(16, 256), full(16, 256), full(8, 128), full(16, 8, 128),
            half(256, 1024), half(16, 16, 1024), half(16, 16, 1024), half(256, 1024),
            full(256, 256), full(256, 1024), full(256, 1024), full(256, 1024),
            half(2, 4, 1024, 256), half(2, 1024, 1024), half(2, 4, 4, 128, 512), half(2, 4, 4, 128, 512), half(2, 4, 128, 256),
            dma((12,)), dma((3,)), dma((3,)), dma((2,)), dma((2,)), dma((2,)),
            dma((2,)), dma, dma((2,)), dma, dma((2,)), dma, dma((7, 3)), dma((2,)), dma((2, 8)), dma, dma((3, 7, 3)), dma((2,)),
        ],
        compiler_params=pltpu.CompilerParams(
            collective_id=0, has_side_effects=True, vmem_limit_bytes=56 * 2**20
        ),
    )(
        x_in[0], b_in[0], c_in[0], z_in[0], dt_raw[0], conv_x[0], conv_b[0], conv_c[0],
        a_rate, dt_bias, skip_d, norm_gain, out_weight[0],
    )
    return mixed[None]


def solution(mesh):
    finer = Mesh(
        mesh.devices.reshape(mesh.shape["section"], 4, 4, mesh.shape["head"]),
        ("section", "seq_0", "seq_1", "head"),
    )
    return jax.shard_map(
        per_device,
        mesh=finer,
        in_specs=(
            P("section", SEQ, "head"),
            P("section", SEQ, "head"),
            P("section", SEQ, "head"),
            P("section", SEQ, "head"),
            P("section", "head", SEQ),
            P("section", None, "head"),
            P("section", None, "head"),
            P("section", None, "head"),
            P("section", "head"),
            P("section", "head"),
            P("section", "head"),
            P("section", "head"),
            P("section", "head", SEQ),
        ),
        out_specs=P("section", SEQ_HEAD, None),
        check_vma=False,
    )
```
